32 devices in a mesh: section: 4 (over z), dp: 8 (over y, x, core).
Axes of the slice: x: 2, y: 2, z: 4, core: 2. Of those that a mesh axis runs over, the one named last changes fastest.
Arguments:
- inputs: bfloat16 [2048, 2048], P('dp'), may hold values from -6 to 6
- order: int32 [8, 2], P('dp'), may hold values from 0 to 1, each once within a row
- image_start: int32 [8, 2], P('dp'), may hold values from 0 to 112, as said below
- image_len: int32 [8, 2], P('dp'), may hold values from 16 to 64
- norm_gain: float32 [4, 2048], P('section'), may hold values from 0.25 to 1.75
- qkv_weight: bfloat16 [4, 2048, 6144], P('section', 'dp'), may hold values from -0.125 to 0.125
- q_gain: float32 [4, 2048], P('section'), may hold values from 0.5 to 2.5
- k_gain: float32 [4, 2048], P('section'), may hold values from 0.5 to 2.5
- o_weight: bfloat16 [4, 2048, 2048], P('section'), may hold values from -0.125 to 0.125
Outputs:
- section_outputs: bfloat16 [4, 2048, 2048], P('section', 'dp')
The draws below stay inside these ranges and needn't reach their ends.
Inputs may be any that keep to these rules, and one draw needn't show every extreme that they name: `order`: each row is a permutation of the micro-batch numbers. image_start + image_len <= 128 for every micro-batch.
All inputs are finite; a program needn't handle non-finite values.
Results may differ from the reference program's by a relative error of at most 0.035.
Values may be sent and summed in bfloat16 or wider, within the bound.
A program may use at most 128 MiB of HBM per device.

```python
import math
import jax
import jax.numpy as jnp
from jax import lax

HEADS = 16
HEAD_DIM = 128
SEQ = 128
MICRO = 2
D = 2048
TOKENS = 2048
N_SECTION = 4
N_DP = 8


def span_pair(key):
    folded = jax.random.fold_in(key, 7)
    shortest = max(1, SEQ // 8)
    longest = SEQ // 2
    length = jax.random.randint(jax.random.fold_in(folded, 1), (N_DP, MICRO), shortest, longest + 1)
    random_bits = jax.random.randint(jax.random.fold_in(folded, 2), (N_DP, MICRO), 0, 1 << 20)
    chosen_group = jax.random.randint(jax.random.fold_in(folded, 3), (), 0, N_DP)
    chosen_micro = jax.random.randint(jax.random.fold_in(folded, 4), (), 0, MICRO)
    second_micro = (chosen_micro + 1) % MICRO
    group_index = jnp.arange(N_DP, dtype=jnp.int32)[:, None]
    micro_index = jnp.arange(MICRO, dtype=jnp.int32)[None, :]
    at_end = (group_index == chosen_group) & (micro_index == chosen_micro)
    at_long = (group_index == chosen_group) & (micro_index == second_micro)
    length = jnp.where(at_end, shortest, jnp.where(at_long, longest, length))
    start = random_bits % (SEQ - length + 1)
    start = jnp.where(at_end, SEQ - shortest, start)
    return (start.astype(jnp.int32), length.astype(jnp.int32))


def draw_image_start(key, part):
    return span_pair(key)[0]


def draw_image_len(key, part):
    return span_pair(key)[1]


def level_of(rng, shape, pieces, low, high):
    level, own = 1.0, jax.random.fold_in(rng, 6)
    for axis_at, shards_of in pieces:
        heights = jnp.exp(jax.random.uniform(jax.random.fold_in(own, axis_at), (shards_of,), jnp.float32, low / len(pieces), high / len(pieces)))
        level = level * jnp.repeat(heights, shape[axis_at] // shards_of).reshape([-1 if axis == axis_at else 1 for axis in range(len(shape))])
    return level


def scatter_about(stream_key, dims, deviation, most, cuts=(), kind=jnp.bfloat16):
    entries = deviation * jax.random.normal(stream_key, dims, jnp.float32)
    if cuts:
        entries = entries * level_of(stream_key, dims, cuts, -0.22, 0.18)
    return jnp.clip(entries, -most, most).astype(kind)


def setup_inputs(seed: int = 0) -> dict:
    keys = jax.random.split(jax.random.key(seed), 10)
    inputs = scatter_about(keys[0], (TOKENS, D), 1.0, 6.0, ((0, 8),))
    order = jax.vmap(lambda own: jax.random.permutation(own, MICRO))(jax.random.split(keys[1], N_DP)).reshape((N_DP, MICRO)).astype(jnp.int32)
    image_start = draw_image_start(jax.random.fold_in(keys[9], 71), 0)
    image_len = draw_image_len(jax.random.fold_in(keys[9], 71), 0)
    norm_gain = jnp.clip(1.0 + 0.15 * jax.random.normal(keys[4], (N_SECTION, D), jnp.float32), 0.25, 1.75)
    qkv_weight = scatter_about(keys[5], (N_SECTION, D, 3 * D), D ** -0.5, 0.125, ((0, 4), (1, 8)))
    q_gain = jnp.clip(jnp.exp(math.log(2.5) - 1.609438 * jax.random.uniform(keys[6], (N_SECTION, D), jnp.float32) ** level_of(keys[6], (N_SECTION, D), ((0, 4),), -0.2, 0.2)), 0.5, 2.5)
    k_gain = jnp.clip(jnp.exp(math.log(2.5) - 1.609438 * jax.random.uniform(keys[7], (N_SECTION, D), jnp.float32) ** level_of(keys[7], (N_SECTION, D), ((0, 4),), -0.2, 0.2)), 0.5, 2.5)
    o_weight = scatter_about(keys[8], (N_SECTION, D, D), D ** -0.5, 0.125, ((0, 4),))
    return dict(inputs=inputs, order=order, image_start=image_start, image_len=image_len, norm_gain=norm_gain, qkv_weight=qkv_weight, q_gain=q_gain, k_gain=k_gain, o_weight=o_weight)


epsilon_value = 1e-05

def normalize(hidden, gain):
    widened = hidden.astype(jnp.float32)
    mean_square = lax.optimization_barrier(jnp.mean(widened * widened, axis=-1, keepdims=True))
    return (widened * lax.rsqrt(mean_square + epsilon_value) * gain).astype(jnp.bfloat16)

def head_norm(block, gain, seq_len):
    split = block.reshape(seq_len, HEADS, HEAD_DIM)
    mean_square = lax.optimization_barrier(jnp.mean(split * split, axis=-1, keepdims=True))
    return (split * lax.rsqrt(mean_square + epsilon_value) * gain.reshape(HEADS, HEAD_DIM)).astype(jnp.bfloat16)

def finish(hidden, projected, gain_query, gain_key, out_weight, start, length):
    seq_len, model_width = hidden.shape
    queries = head_norm(projected[:, :model_width], gain_query, seq_len)
    key_rows = head_norm(projected[:, model_width:2 * model_width], gain_key, seq_len)
    value_rows = projected[:, 2 * model_width:].astype(jnp.bfloat16).reshape(seq_len, HEADS, HEAD_DIM)
    scores = jnp.einsum('qhd,khd->hqk', queries.astype(jnp.float32), key_rows.astype(jnp.float32)) * HEAD_DIM ** (-0.5)
    position = jnp.arange(seq_len, dtype=jnp.int32)
    in_image = (position >= start) & (position < start + length)
    allowed = (position[None, :] <= position[:, None]) | in_image[:, None] & in_image[None, :]
    scores = jnp.where(allowed[None], scores, -1e+30)
    row_max = lax.optimization_barrier(jnp.max(scores, axis=-1, keepdims=True))
    lifted = jnp.exp(scores - row_max)
    probabilities = (lifted / lax.optimization_barrier(jnp.sum(lifted, axis=-1, keepdims=True))).astype(jnp.bfloat16)
    mixed = jnp.einsum('hqk,khd->qhd', probabilities.astype(jnp.float32), value_rows.astype(jnp.float32))
    attended = mixed.reshape(seq_len, model_width).astype(jnp.bfloat16)
    output_rows = jnp.dot(attended, out_weight, preferred_element_type=jnp.float32)
    return (hidden.astype(jnp.float32) + output_rows).astype(jnp.bfloat16)

def reference(inputs, order, image_start, image_len, norm_gain, qkv_weight, q_gain, k_gain, o_weight):
    groups = inputs.reshape(N_DP, MICRO, SEQ, D)

    def one_group(packed):
        states, permutation, starts, lengths = packed
        states = states[permutation.astype(jnp.int32)]
        starts = starts[permutation.astype(jnp.int32)]
        lengths = lengths[permutation.astype(jnp.int32)]
        collected = []
        for section_number in range(N_SECTION):
            normed = normalize(states.reshape(MICRO * SEQ, D), norm_gain[section_number])
            projected = jnp.dot(normed, qkv_weight[section_number], preferred_element_type=jnp.float32)
            projected = projected.reshape(MICRO, SEQ, 3 * D)
            gain_query = q_gain[section_number]
            gain_key = k_gain[section_number]
            out_weight = o_weight[section_number]
            states = jax.vmap(lambda one, proj_rows, first, count: finish(one, proj_rows, gain_query, gain_key, out_weight, first, count))(states, projected, starts, lengths)
            collected.append(states)
        return jnp.stack(collected)
    result = lax.map(one_group, (groups, order, image_start, image_len))
    return jnp.transpose(result, (1, 0, 2, 3, 4)).reshape(N_SECTION, N_DP * MICRO * SEQ, D)
```

```python
import functools
import jax
import jax.numpy as jnp
from jax import lax
from jax.experimental import pallas as pl
from jax.experimental.pallas import tpu as pltpu
from jax.sharding import PartitionSpec as P

HEAD_DIM = 128
EPS = 1e-05
LOG2_E = 1.4426950408889634
SUBS = 2
CHUNKS = 4
WIDE = 1
HEADS_AT_ONCE = 16
NORMS_AT_ONCE = 16
SHARED_SECTIONS = 2
PARTS = 3
MESH = pl.DeviceIdType.MESH


def grid_of(chips):
    columns = 1
    while columns * columns < chips:
        columns *= 2
    return chips // columns, columns


def ring_order(chips):
    rows, columns = grid_of(chips)
    cells = []
    for r in range(rows):
        line = list(range(1, columns))
        cells += [r * columns + c for c in (line if r % 2 == 0 else line[::-1])]
    cells += [r * columns for r in reversed(range(rows))]
    return cells


def look(table, index):
    found = jnp.int32(0)
    for i, value in enumerate(table):
        found = found + jnp.where(index == i, jnp.int32(value), jnp.int32(0))
    return found


def flip(value):
    return value + 1 - 2 * lax.rem(value, 2)


def aligned(start, size):
    return pl.ds(start if isinstance(start, int) else pl.multiple_of(start, size), size)


def kernel(
    sections, devices,
    order_ref, start_ref, len_ref, x_ref, gain_ref, w_ref, qg_ref, kg_ref, o_ref,
    out_ref,
    wbuf, obuf, xin, xout, acc, qkv, att, xmate, ret, ssq, spans, mate_spans,
    own_sem, o_sem, first_send, first_recv, ring_send, ring_recv, pair_send, pair_recv,
    hop_send, hop_recv,
    own_sems, swap_send, swap_recv, loop_send, loop_recv, core_send, core_recv,
    mine_send, mine_recv, x_send, x_recv, give_send, give_recv, span_send, span_recv,
):
    chips = devices // 2
    grid_rows, columns = grid_of(chips)
    order = ring_order(chips)
    inverse = [order.index(c) for c in range(chips)]
    shard, total = w_ref.shape
    piece = shard // (2 * SUBS)
    micro, chunks, seq, width = xin.shape
    model = chunks * width
    quarter = model // 4
    few = quarter // HEAD_DIM
    sec = lax.axis_index("section")
    me = lax.axis_index("dp")
    core = lax.rem(me, 2)
    chip = lax.div(me, 2)
    place = look(inverse, chip)
    partner = flip(me)

    def at(offset):
        return look(order, lax.rem(place + (offset % chips), chips)) * 2 + core

    ahead, behind = at(1), at(-1)
    above = lax.rem(sec + 1, sections)
    below = lax.rem(sec + sections - 1, sections)

    row, col = lax.div(chip, columns), lax.rem(chip, columns)
    across, down = lax.rem(col, 2), lax.rem(row, 2)
    units = (across, 2 + down)
    half_c, half_r = columns // 2, grid_rows // 2
    places = (row * half_c + lax.div(col, 2), col * half_r + lax.div(row, 2))
    length = chips // 2

    def device(r, c):
        return (r * columns + c) * 2 + core

    mates = (device(row, flip(col)), device(flip(row), col))

    def seat(s, offset, mate):
        spot = lax.rem(places[s] + (offset % length), length)
        if s == 0:
            r, c = lax.div(spot, half_c), 2 * lax.rem(spot, half_c) + across
            c = flip(c) if mate else c
        else:
            c, r = lax.div(spot, half_r), 2 * lax.rem(spot, half_r) + down
            r = flip(r) if mate else r
        return device(r, c)

    def block(owner):
        return aligned(owner * shard, shard)

    def cols_of(unit, part):
        return aligned(part * model + unit * quarter, quarter)

    shared = sec < SHARED_SECTIONS

    def stay(s, p):
        where = cols_of(units[s], p)
        return pltpu.make_async_copy(w_ref.at[:, where], wbuf.at[block(me), where], own_sems.at[s, p])

    o_copy = pltpu.make_async_copy(o_ref, obuf, o_sem)
    own_rows = block(me)
    own = pltpu.make_async_copy(w_ref, wbuf.at[own_rows], own_sem)

    @pl.when(shared)
    def _():
        for s in range(2):
            for p in range(PARTS):
                stay(s, p).start()
        for j in range(micro):
            which = order_ref[0, j]
            s0 = start_ref[0, which]
            spans[j, 0] = jnp.full(spans.shape[2:], s0, jnp.int32)
            spans[j, 1] = jnp.full(spans.shape[2:], s0 + len_ref[0, which], jnp.int32)

            @pl.when(sec == 0)
            def _():
                for c in range(chunks):
                    xin[j, c] = x_ref[which, :, c * width : (c + 1) * width]

    @pl.when(jnp.logical_not(shared))
    def _():
        own.start()

    o_copy.start()

    barrier = pltpu.get_barrier_semaphore()
    near = [mates[0], mates[1], partner]
    if chips > 4:
        near += [ahead, behind]
        for s in range(2):
            near += [seat(s, 1, False), seat(s, -1, False)]
    for other in near:
        pl.semaphore_signal(barrier, inc=1, device_id=(sec, other), device_id_type=MESH)

    @pl.when(sec < sections - 1)
    def _():
        pl.semaphore_signal(barrier, inc=1, device_id=(above, me), device_id_type=MESH)

    @pl.when(sec > 0)
    def _():
        pl.semaphore_signal(barrier, inc=1, device_id=(below, me), device_id_type=MESH)

    line = (sec > 0).astype(jnp.int32) + (sec < sections - 1).astype(jnp.int32)
    pl.semaphore_wait(barrier, len(near) + line)

    def hop(j, c):
        return pltpu.make_async_remote_copy(
            src_ref=xout.at[j, c], dst_ref=xin.at[j, c],
            send_sem=hop_send.at[j, c], recv_sem=hop_recv.at[j, c],
            device_id=(above, me), device_id_type=MESH,
        )

    row_id = lax.broadcasted_iota(jnp.int32, (seq, seq), 0)
    col_id = lax.broadcasted_iota(jnp.int32, (seq, seq), 1)

    def mask(s0, s1):
        return (col_id <= row_id) | (
            (row_id >= s0) & (row_id < s1) & (col_id >= s0) & (col_id < s1)
        )

    def leave(j):
        for c in range(chunks):
            span = slice(c * width, (c + 1) * width)
            grown = jnp.dot(att[j], obuf[:, span], preferred_element_type=jnp.float32)
            fresh = (xin[j, c].astype(jnp.float32) + grown).astype(jnp.bfloat16)
            xout[j, c] = fresh
            out_ref[j, :, span] = fresh

            @pl.when(sec < sections - 1)
            def _():
                hop(j, c).start()

    def head(q, k, v, allowed):
        scores = lax.dot_general(
            q, k, (((1,), (1,)), ((), ())), preferred_element_type=jnp.float32
        )
        lifted = jnp.where(allowed, jnp.exp2(scores), 0.0)
        mixed = jnp.dot(
            lifted.astype(jnp.bfloat16), v.astype(jnp.bfloat16),
            preferred_element_type=jnp.float32,
        )
        return (mixed * (1.0 / jnp.sum(lifted, axis=-1, keepdims=True))).astype(jnp.bfloat16)

    def lifted_norm(p, scale, gain):
        mean = jnp.mean(p * p, axis=-1, keepdims=True) * scale * scale
        return (p * (lax.rsqrt(mean + EPS) * scale) * gain).astype(jnp.bfloat16)

    @pl.when(shared)
    def _():
        def remote(source, dest, sent, got, other):
            return pltpu.make_async_remote_copy(
                src_ref=source, dst_ref=dest, send_sem=sent, recv_sem=got,
                device_id=(sec, other), device_id_type=MESH,
            )

        def swap(s, p):
            where = cols_of(flip(units[s]), p)
            return remote(
                w_ref.at[:, where], wbuf.at[own_rows, where],
                swap_send.at[s, p], swap_recv.at[s, p], mates[s],
            )

        def circle(s, k, b, p):
            where = cols_of(units[s], p)
            rows = block(seat(s, 1 - k, b == 1))
            source = w_ref.at[:, where] if k == 1 and b == 0 else wbuf.at[rows, where]
            return remote(
                source, wbuf.at[rows, where],
                loop_send.at[s, k - 1, b, p], loop_recv.at[s, k - 1, b, p], seat(s, 1, False),
            )

        def owner_of(s, i):
            return mates[s] if i == 0 else seat(s, -((i + 1) // 2), i % 2 == 0)

        def hand(s, i, p):
            here = wbuf.at[block(owner_of(s, i)), cols_of(units[s], p)]
            return remote(here, here, core_send.at[s, i, p], core_recv.at[s, i, p], partner)

        def mine(s, p):
            where = cols_of(units[s], p)
            return remote(
                w_ref.at[:, where], wbuf.at[own_rows, where],
                mine_send.at[s, p], mine_recv.at[s, p], partner,
            )

        def share(s, j, c):
            return remote(
                xin.at[j, c], xmate.at[s, j, c], x_send.at[s, j, c], x_recv.at[s, j, c], mates[s]
            )

        def give(s, j):
            return remote(
                ret.at[s, j], att.at[j, :, aligned(units[s] * quarter, quarter)],
                give_send.at[s, j], give_recv.at[s, j], mates[s],
            )

        def tell(s):
            return remote(spans, mate_spans.at[s], span_send.at[s], span_recv.at[s], mates[s])

        both = [(p, s) for p in range(PARTS) for s in range(2)]
        waves = 2 * length - 1

        for s in range(2):
            tell(s).start()

        @pl.when(sec == 0)
        def _():
            for c in range(chunks):
                for s in range(2):
                    share(s, 0, c).start()

        for p, s in both:
            swap(s, p).start()
        for p, s in both:
            mine(s, p).start()
        for p, s in both:
            circle(s, 1, 0, p).start()

        def fold(x):
            out = x[:, :128]
            for i in range(1, x.shape[1] // 128):
                out = out + x[:, i * 128 : (i + 1) * 128]
            return out

        def take(ref, j, start, size):
            if isinstance(start, int):
                return ref[j, start // width, :, start % width : start % width + size]
            if size == width:
                return ref[j, lax.div(start, width)]
            return ref[j, lax.div(start, width), :, aligned(lax.rem(start, width), size)]

        def project(j, s, start, size, parts, fresh):
            here = aligned(start, size)
            gain = gain_ref[:, here]
            ours = take(xin, j, start, size).astype(jnp.float32)
            theirs = take(xmate.at[s], j, start, size).astype(jnp.float32)
            left = jnp.concatenate(
                [(ours * gain).astype(jnp.bfloat16), (theirs * gain).astype(jnp.bfloat16)], axis=0
            )
            for p in parts:
                cols = cols_of(units[s], p)
                part = jnp.dot(left, wbuf[here, cols], preferred_element_type=jnp.float32)
                if fresh:
                    acc[:, cols] = part
                else:
                    acc[:, cols] += part
            if 0 in parts:
                squares = [(1 + s, theirs)] + ([(0, ours)] if s == 0 else [])
                for k, x in squares:
                    if fresh:
                        ssq[k] = fold(x * x)
                    else:
                        ssq[k] += fold(x * x)

        chip_rows = 2 * shard

        @pl.when(sec == 0)
        def _():
            for c in range(chunks):
                for s in range(2):
                    share(s, 0, c).wait_recv()

        for p, s in both:
            stay(s, p).wait()
            mine(s, p).wait_recv()

        @pl.when(sec == 0)
        def _():
            for s in range(2):
                project(0, s, chip * chip_rows, chip_rows, range(PARTS), True)

        for i in range(waves):
            def finish(p):
                for s in range(2):
                    hand(s, i, p).wait_recv()

                @pl.when(sec == 0)
                def _():
                    for s in range(2):
                        start = lax.div(owner_of(s, i), 2) * chip_rows
                        project(0, s, start, chip_rows, (p,), False)

            for p in range(PARTS):
                for s in range(2):
                    if i == 0:
                        swap(s, p).wait_recv()
                        circle(s, 1, 1, p).start()
                    else:
                        k, b = (i + 1) // 2, (i + 1) % 2
                        circle(s, k, b, p).wait_recv()
                        if k < length - 1:
                            circle(s, k + 1, b, p).start()
                    hand(s, i, p).start()
                if p > 0:
                    finish(p - 1)
            finish(PARTS - 1)

        for s in range(2):
            tell(s).wait_recv()
        o_copy.wait()

        def attend(turn, region, unit, scale, allowed, ref, base):
            rows = slice(region * seq, (region + 1) * seq)
            for part, gains in ((0, qg_ref), (1, kg_ref)):
                factor = HEAD_DIM ** (-0.5) * LOG2_E if part == 0 else 1.0
                for i in range(few):
                    start = unit * quarter + i * HEAD_DIM
                    p = acc[rows, aligned(part * model + start, HEAD_DIM)]
                    spot = (turn * 2 + part) * quarter + i * HEAD_DIM
                    qkv[:, spot : spot + HEAD_DIM] = lifted_norm(
                        p, scale, gains[:, aligned(start, HEAD_DIM)] * factor
                    )
            for i in range(few):
                spot = turn * 2 * quarter + i * HEAD_DIM
                v = acc[rows, aligned(2 * model + unit * quarter + i * HEAD_DIM, HEAD_DIM)] * scale
                ref[:, aligned(base + i * HEAD_DIM, HEAD_DIM)] = head(
                    qkv[:, spot : spot + HEAD_DIM],
                    qkv[:, spot + quarter : spot + quarter + HEAD_DIM], v, allowed,
                )

        @pl.loop(0, micro)
        def _(j):
            @pl.when((sec > 0) | (j > 0))
            def _():
                def finish(c):
                    for s in range(2):
                        share(s, j, c).wait_recv()
                    for s in range(2):
                        project(j, s, c * width, width, range(PARTS), c == 0)

                for c in range(chunks):
                    @pl.when(sec > 0)
                    def _():
                        hop(j, c).wait_recv()
                        for s in range(2):
                            share(s, j, c).start()

                    if c > 0:
                        finish(c - 1)
                finish(chunks - 1)

            def scale_of(k):
                square = jnp.sum(ssq[k], axis=-1, keepdims=True)
                return lax.rsqrt(square * (1.0 / model) + EPS)

            for s in range(2):
                allowed = mask(mate_spans[s, j, 0, 0:1, :], mate_spans[s, j, 1, 0:1, :])
                attend(s, 1, units[s], scale_of(1 + s), allowed, ret.at[s, j], 0)
                give(s, j).start()

            @pl.when((sec == 0) & (j < micro - 1))
            def _():
                for c in range(chunks):
                    for s in range(2):
                        share(s, j + 1, c).start()

            which = order_ref[0, j]
            s0 = start_ref[0, which]
            allowed = mask(s0, s0 + len_ref[0, which])
            scale = scale_of(0)
            for s in range(2):
                attend(2 + s, 0, units[s], scale, allowed, att.at[j], units[s] * quarter)
            for s in range(2):
                give(s, j).wait_recv()
            leave(j)

        for s in range(2):
            tell(s).wait_send()
            for p in range(PARTS):
                swap(s, p).wait_send()
                mine(s, p).wait_send()
                for i in range(waves):
                    hand(s, i, p).wait_send()
                for k in range(1, length):
                    for b in range(2):
                        circle(s, k, b, p).wait_send()
            for j in range(micro):
                give(s, j).wait_send()
                for c in range(chunks):
                    share(s, j, c).wait_send()

    @pl.when(jnp.logical_not(shared))
    def _():
        def rows(owner, way, sub):
            return pl.ds(pl.multiple_of(owner * shard + (way * SUBS + sub) * piece, piece), piece)

        def ring_copy(way, sub, step):
            owner = at(-step if way == 0 else step)
            where = rows(owner, way, sub)
            if step == 0:
                source = w_ref.at[pl.ds((way * SUBS + sub) * piece, piece)]
            else:
                source = wbuf.at[where]
            return pltpu.make_async_remote_copy(
                src_ref=source, dst_ref=wbuf.at[where],
                send_sem=ring_send.at[way, sub, step], recv_sem=ring_recv.at[way, sub, step],
                device_id=(sec, ahead if way == 0 else behind), device_id_type=MESH,
            )

        def pair_copy(way, sub, step):
            owner = at(-step if way == 0 else step)
            where = rows(owner, way, sub)
            return pltpu.make_async_remote_copy(
                src_ref=wbuf.at[where], dst_ref=wbuf.at[where],
                send_sem=pair_send.at[way, sub, step - 1], recv_sem=pair_recv.at[way, sub, step - 1],
                device_id=(sec, partner), device_id_type=MESH,
            )

        ring = {}
        pair = {}
        for sub in range(SUBS):
            for way in range(2):
                ring[way, sub, 0] = ring_copy(way, sub, 0)
                ring[way, sub, 0].start()
        first = pltpu.make_async_remote_copy(
            src_ref=w_ref, dst_ref=wbuf.at[own_rows], send_sem=first_send, recv_sem=first_recv,
            device_id=(sec, partner), device_id_type=MESH,
        )
        first.start()
        own.wait()
        first.wait_recv()
        for step in range(1, chips):
            for sub in range(SUBS):
                for way in range(2):
                    ring[way, sub, step - 1].wait_recv()
                    if step < chips - 1:
                        ring[way, sub, step] = ring_copy(way, sub, step)
                        ring[way, sub, step].start()
                    pair[way, sub, step] = pair_copy(way, sub, step)
                    pair[way, sub, step].start()
            for way in range(2):
                for sub in range(SUBS):
                    pair[way, sub, step].wait_recv()
        o_copy.wait()
        first.wait_send()
        for step in range(1, chips):
            for sub in range(SUBS):
                for way in range(2):
                    pair[way, sub, step].wait_send()
                    ring[way, sub, step - 1].wait_send()

        @pl.loop(0, micro)
        def _(j):
            which = order_ref[0, j]
            s0 = start_ref[0, which]
            s1 = s0 + len_ref[0, which]
            here_rows = slice(0, seq)
            square = jnp.zeros((seq, 1), jnp.float32)
            for c in range(chunks):
                span = slice(c * width, (c + 1) * width)
                hop(j, c).wait_recv()
                wide = xin[j, c].astype(jnp.float32)
                square = square + jnp.sum(wide * wide, axis=-1, keepdims=True)
                scaled = (wide * gain_ref[:, span]).astype(jnp.bfloat16)

                @pl.loop(0, WIDE)
                def _(n):
                    cols = pl.ds(pl.multiple_of(n * (total // WIDE), total // WIDE), total // WIDE)
                    part = jnp.dot(scaled, wbuf[span, cols], preferred_element_type=jnp.float32)
                    if c == 0:
                        acc[here_rows, cols] = part
                    else:
                        acc[here_rows, cols] += part

            scale = lax.rsqrt(square * (1.0 / model) + EPS)

            for part, gains in ((0, qg_ref), (1, kg_ref)):
                factor = HEAD_DIM ** (-0.5) * LOG2_E if part == 0 else 1.0

                @pl.loop(0, model // (NORMS_AT_ONCE * HEAD_DIM))
                def _(n):
                    for i in range(NORMS_AT_ONCE):
                        base = (n * NORMS_AT_ONCE + i) * HEAD_DIM
                        here = pl.ds(pl.multiple_of(base, HEAD_DIM), HEAD_DIM)
                        cols = pl.ds(pl.multiple_of(part * model + base, HEAD_DIM), HEAD_DIM)
                        qkv[:, cols] = lifted_norm(acc[here_rows, cols], scale, gains[:, here] * factor)

            allowed = mask(s0, s1)

            @pl.loop(0, model // (HEADS_AT_ONCE * HEAD_DIM))
            def _(n):
                for i in range(HEADS_AT_ONCE):
                    base = (n * HEADS_AT_ONCE + i) * HEAD_DIM
                    here = pl.ds(pl.multiple_of(base, HEAD_DIM), HEAD_DIM)
                    q = qkv[:, here]
                    k = qkv[:, pl.ds(pl.multiple_of(model + base, HEAD_DIM), HEAD_DIM)]
                    v = acc[here_rows, pl.ds(pl.multiple_of(2 * model + base, HEAD_DIM), HEAD_DIM)] * scale
                    att[j, :, here] = head(q, k, v, allowed)

            leave(j)

    @pl.when(sec < sections - 1)
    def _():
        for j in range(micro):
            for c in range(chunks):
                hop(j, c).wait_send()


def solution(mesh):
    sections, devices = mesh.shape["section"], mesh.shape["dp"]

    def body(inputs, order, image_start, image_len, norm_gain, qkv_weight, q_gain, k_gain, o_weight):
        micro = order.shape[1]
        count, model = inputs.shape
        seq = count // micro
        total = qkv_weight.shape[2]
        shard = qkv_weight.shape[1]
        width = model // CHUNKS
        chunks = model // width
        chips = devices // 2
        length = chips // 2
        smem = pl.BlockSpec(memory_space=pltpu.SMEM)
        vmem = pl.BlockSpec(memory_space=pltpu.VMEM)
        hbm = pl.BlockSpec(memory_space=pltpu.HBM)
        dma = pltpu.SemaphoreType.DMA
        out = pl.pallas_call(
            functools.partial(kernel, sections, devices),
            out_shape=jax.ShapeDtypeStruct((micro, seq, model), jnp.bfloat16),
            in_specs=[smem, smem, smem, vmem, vmem, hbm, vmem, vmem, hbm],
            out_specs=vmem,
            scratch_shapes=[
                pltpu.VMEM((model, total), jnp.bfloat16),
                pltpu.VMEM((model, model), jnp.bfloat16),
                pltpu.VMEM((micro, chunks, seq, width), jnp.bfloat16),
                pltpu.VMEM((micro, chunks, seq, width), jnp.bfloat16),
                pltpu.VMEM((2 * seq, total), jnp.float32),
                pltpu.VMEM((seq, 2 * model), jnp.bfloat16),
                pltpu.VMEM((micro, seq, model), jnp.bfloat16),
                pltpu.VMEM((2, micro, chunks, seq, width), jnp.bfloat16),
                pltpu.VMEM((2, micro, seq, model // 4), jnp.bfloat16),
                pltpu.VMEM((3, seq, 128), jnp.float32),
                pltpu.VMEM((micro, 2, 8, 128), jnp.int32),
                pltpu.VMEM((2, micro, 2, 8, 128), jnp.int32),
                dma, dma, dma, dma,
                dma((2, SUBS, chips - 1)),
                dma((2, SUBS, chips - 1)),
                dma((2, SUBS, chips - 1)),
                dma((2, SUBS, chips - 1)),
                dma((micro, chunks)),
                dma((micro, chunks)),
                dma((2, PARTS)),
                dma((2, PARTS)),
                dma((2, PARTS)),
                dma((2, length - 1, 2, PARTS)),
                dma((2, length - 1, 2, PARTS)),
                dma((2, 2 * length - 1, PARTS)),
                dma((2, 2 * length - 1, PARTS)),
                dma((2, PARTS)),
                dma((2, PARTS)),
                dma((2, micro, chunks)),
                dma((2, micro, chunks)),
                dma((2, micro)),
                dma((2, micro)),
                dma((2,)),
                dma((2,)),
            ],
            compiler_params=pltpu.CompilerParams(
                collective_id=0, has_side_effects=True, vmem_limit_bytes=60 * 1024 * 1024
            ),
        )(
            order, image_start, image_len, inputs.reshape(micro, seq, model), norm_gain,
            qkv_weight.reshape(shard, total), q_gain, k_gain, o_weight.reshape(model, model),
        )
        return out.reshape(1, count, model)

    in_specs = (
        P("dp", None),
        P("dp", None),
        P("dp", None),
        P("dp", None),
        P("section", None),
        P("section", "dp", None),
        P("section", None),
        P("section", None),
        P("section", None, None),
    )
    out_specs = P("section", "dp", None)
    return jax.shard_map(body, mesh=mesh, in_specs=in_specs, out_specs=out_specs, check_vma=False)
```

```python
import functools
import jax
import jax.numpy as jnp
from jax import lax
from jax.experimental import pallas as pl
from jax.experimental.pallas import tpu as pltpu
from jax.sharding import PartitionSpec as P

HEAD_DIM = 128
EPS = 1e-05
LOG2_E = 1.4426950408889634
SUBS = 2
CHUNKS = 8
GROUP = 2
LAG = 3
EARLY = ((2, 2, 1, 1), (0, 2, 1, 1))
HEADS_AT_ONCE = 16
NORMS_AT_ONCE = 16
SHARED_SECTIONS = 3
PARTS = 3
RETURNS = 2
MESH = pl.DeviceIdType.MESH


def grid_of(chips):
    columns = 1
    while columns * columns < chips:
        columns *= 2
    return chips // columns, columns


def ring_order(chips):
    rows, columns = grid_of(chips)
    cells = []
    for r in range(rows):
        line = list(range(1, columns))
        cells += [r * columns + c for c in (line if r % 2 == 0 else line[::-1])]
    cells += [r * columns for r in reversed(range(rows))]
    return cells


def look(table, index):
    found = jnp.int32(0)
    for i, value in enumerate(table):
        found = found + jnp.where(index == i, jnp.int32(value), jnp.int32(0))
    return found


def flip(value):
    return value + 1 - 2 * lax.rem(value, 2)


def aligned(start, size):
    return pl.ds(start if isinstance(start, int) else pl.multiple_of(start, size), size)


def kernel(
    sections, devices,
    order_ref, start_ref, len_ref, x_ref, gain_ref, w_ref, qg_ref, kg_ref, o_ref,
    out_ref,
    wbuf, obuf, xin, xout, acc, qkv, att, xmate, relay, ret, ssq, spans, mate_spans,
    own_sem, o_sem, first_send, first_recv, ring_send, ring_recv, pair_send, pair_recv,
    hop_send, hop_recv,
    own_sems, swap_send, swap_recv, loop_send, loop_recv, core_send, core_recv,
    mine_send, mine_recv, x_send, x_recv, give_send, give_recv, span_send, span_recv,
    pass_send, pass_recv, fall_send, out_sem,
):
    chips = devices // 2
    grid_rows, columns = grid_of(chips)
    order = ring_order(chips)
    inverse = [order.index(c) for c in range(chips)]
    shard, total = w_ref.shape
    piece = shard // (2 * SUBS)
    micro, seq, model = xin.shape
    chunks, width = CHUNKS, model // CHUNKS
    quarter = model // 4
    few = quarter // HEAD_DIM
    sec = lax.axis_index("section")
    me = lax.axis_index("dp")
    core = lax.rem(me, 2)
    chip = lax.div(me, 2)
    place = look(inverse, chip)
    partner = flip(me)

    def at(offset):
        return look(order, lax.rem(place + (offset % chips), chips)) * 2 + core

    ahead, behind = at(1), at(-1)
    above = lax.rem(sec + 1, sections)
    below = lax.rem(sec + sections - 1, sections)

    row, col = lax.div(chip, columns), lax.rem(chip, columns)
    across, down = lax.rem(col, 2), lax.rem(row, 2)
    units = (across, 2 + down)
    half_c, half_r = columns // 2, grid_rows // 2
    places = (row * half_c + lax.div(col, 2), col * half_r + lax.div(row, 2))
    length = chips // 2

    def device(r, c):
        return (r * columns + c) * 2 + core

    mates = (device(row, flip(col)), device(flip(row), col))

    def seat(s, offset, mate):
        spot = lax.rem(places[s] + (offset % length), length)
        if s == 0:
            r, c = lax.div(spot, half_c), 2 * lax.rem(spot, half_c) + across
            c = flip(c) if mate else c
        else:
            c, r = lax.div(spot, half_r), 2 * lax.rem(spot, half_r) + down
            r = flip(r) if mate else r
        return device(r, c)

    def block(owner):
        return aligned(owner * shard, shard)

    def cols_of(unit, part):
        return aligned(part * model + unit * quarter, quarter)

    shared = sec < SHARED_SECTIONS

    def stay(s, p):
        where = cols_of(units[s], p)
        return pltpu.make_async_copy(w_ref.at[:, where], wbuf.at[block(me), where], own_sems.at[s, p])

    o_copy = pltpu.make_async_copy(o_ref, obuf, o_sem)
    own_rows = block(me)
    own = pltpu.make_async_copy(w_ref, wbuf.at[own_rows], own_sem)

    @pl.when(shared)
    def _():
        for s in range(2):
            for p in range(PARTS):
                stay(s, p).start()
        for j in range(micro):
            which = order_ref[0, j]
            s0 = start_ref[0, which]
            spans[j, 0] = jnp.full(spans.shape[2:], s0, jnp.int32)
            spans[j, 1] = jnp.full(spans.shape[2:], s0 + len_ref[0, which], jnp.int32)

            @pl.when(sec == 0)
            def _():
                xin[j] = x_ref[which]

            @pl.when(sec == 1 + j)
            def _():
                xout[j] = x_ref[which]

    @pl.when(jnp.logical_not(shared))
    def _():
        own.start()

    o_copy.start()

    barrier = pltpu.get_barrier_semaphore()
    near = [mates[0], mates[1], partner]
    if chips > 4:
        near += [ahead, behind]
        for s in range(2):
            near += [seat(s, 1, False), seat(s, -1, False)]
    for other in near:
        pl.semaphore_signal(barrier, inc=1, device_id=(sec, other), device_id_type=MESH)

    @pl.when(sec < sections - 1)
    def _():
        pl.semaphore_signal(barrier, inc=1, device_id=(above, me), device_id_type=MESH)

    @pl.when(sec > 0)
    def _():
        pl.semaphore_signal(barrier, inc=1, device_id=(below, me), device_id_type=MESH)

    line = (sec > 0).astype(jnp.int32) + (sec < sections - 1).astype(jnp.int32)
    for j in range(1, micro):
        for here, there in ((0, 1 + j), (1 + j, 0)):
            @pl.when(sec == here)
            def _():
                pl.semaphore_signal(barrier, inc=1, device_id=(there, me), device_id_type=MESH)

            line = line + (sec == here).astype(jnp.int32)
    pl.semaphore_wait(barrier, len(near) + line)

    def span_of(c):
        return pl.ds(c * width, width)

    def hop(j, c):
        return pltpu.make_async_remote_copy(
            src_ref=xout.at[j, :, span_of(c)], dst_ref=xin.at[j, :, span_of(c)],
            send_sem=hop_send.at[j, c], recv_sem=hop_recv.at[j, c],
            device_id=(above, me), device_id_type=MESH,
        )

    row_id = lax.broadcasted_iota(jnp.int32, (seq, seq), 0)
    col_id = lax.broadcasted_iota(jnp.int32, (seq, seq), 1)

    def mask(s0, s1):
        return (col_id <= row_id) | (
            (row_id >= s0) & (row_id < s1) & (col_id >= s0) & (col_id < s1)
        )

    def out(j, g):
        here = (j, slice(None), pl.ds(g * width, GROUP * width))
        return pltpu.make_async_copy(xout.at[here], out_ref.at[here], out_sem.at[j, g // GROUP])

    def leave(j):
        for g in range(0, chunks, GROUP):
            span = slice(g * width, (g + GROUP) * width)
            grown = jnp.dot(att[j], obuf[:, span], preferred_element_type=jnp.float32)
            fresh = (xin[j, :, span].astype(jnp.float32) + grown).astype(jnp.bfloat16)
            xout[j, :, span] = fresh
            out(j, g).start()

            @pl.when(sec < sections - 1)
            def _():
                for c in range(g, g + GROUP):
                    hop(j, c).start()

    def head(q, k, v, allowed):
        scores = lax.dot_general(
            q, k, (((1,), (1,)), ((), ())), preferred_element_type=jnp.float32
        )
        lifted = jnp.where(allowed, jnp.exp2(scores), 0.0)
        mixed = jnp.dot(
            lifted.astype(jnp.bfloat16), v.astype(jnp.bfloat16),
            preferred_element_type=jnp.float32,
        )
        return (mixed * (1.0 / jnp.sum(lifted, axis=-1, keepdims=True))).astype(jnp.bfloat16)

    def lifted_norm(p, scale, gain):
        mean = jnp.mean(p * p, axis=-1, keepdims=True) * scale * scale
        return (p * (lax.rsqrt(mean + EPS) * scale) * gain).astype(jnp.bfloat16)

    @pl.when(shared)
    def _():
        def remote(source, dest, sent, got, other):
            return pltpu.make_async_remote_copy(
                src_ref=source, dst_ref=dest, send_sem=sent, recv_sem=got,
                device_id=(sec, other), device_id_type=MESH,
            )

        def swap(s, p):
            where = cols_of(flip(units[s]), p)
            return remote(
                w_ref.at[:, where], wbuf.at[own_rows, where],
                swap_send.at[s, p], swap_recv.at[s, p], mates[s],
            )

        def circle(s, k, b, p):
            where = cols_of(units[s], p)
            rows = block(seat(s, 1 - k, b == 1))
            source = w_ref.at[:, where] if k == 1 and b == 0 else wbuf.at[rows, where]
            return remote(
                source, wbuf.at[rows, where],
                loop_send.at[s, k - 1, b, p], loop_recv.at[s, k - 1, b, p], seat(s, 1, False),
            )

        def owner_of(s, i):
            return mates[s] if i == 0 else seat(s, -((i + 1) // 2), i % 2 == 0)

        def hand(s, i, p):
            here = wbuf.at[block(owner_of(s, i)), cols_of(units[s], p)]
            return remote(here, here, core_send.at[s, i, p], core_recv.at[s, i, p], partner)

        def mine(s, p):
            where = cols_of(units[s], p)
            return remote(
                w_ref.at[:, where], wbuf.at[own_rows, where],
                mine_send.at[s, p], mine_recv.at[s, p], partner,
            )

        def share(s, j, c):
            return remote(
                xin.at[j, :, span_of(c)], xmate.at[s, j, :, span_of(c)],
                x_send.at[s, j, c], x_recv.at[s, j, c], mates[s],
            )

        def hand_on(s, j, c):
            return remote(
                xout.at[j, :, span_of(c)], relay.at[s, j, :, span_of(c)],
                pass_send.at[s, j, c], pass_recv.at[s, j, c], mates[s],
            )

        def fall(s, j, c):
            return pltpu.make_async_remote_copy(
                src_ref=relay.at[s, j, :, span_of(c)], dst_ref=xmate.at[s, j, :, span_of(c)],
                send_sem=fall_send.at[s, j, c], recv_sem=x_recv.at[s, j, c],
                device_id=(0, me), device_id_type=MESH,
            )

        lot = quarter // RETURNS

        def give(s, j, n):
            return remote(
                ret.at[s, j, :, pl.ds(n * lot, lot)],
                att.at[j, :, aligned(units[s] * quarter + n * lot, lot)],
                give_send.at[s, j, n], give_recv.at[s, j, n], mates[s],
            )

        def tell(s):
            return remote(spans, mate_spans.at[s], span_send.at[s], span_recv.at[s], mates[s])

        both = [(p, s) for p in range(PARTS) for s in range(2)]
        waves = 2 * length - 1

        for s in range(2):
            tell(s).start()

        for j in range(micro):
            @pl.when(sec == 1 + j)
            def _():
                for c in range(chunks):
                    for s in range(2):
                        hand_on(s, j, c).start()

        for p, s in both:
            swap(s, p).start()
        for p, s in both:
            mine(s, p).start()
        for p, s in both:
            circle(s, 1, 0, p).start()

        def fold(x):
            out = x[:, :128]
            for i in range(1, x.shape[1] // 128):
                out = out + x[:, i * 128 : (i + 1) * 128]
            return out

        def project(j, s, start, size, parts, fresh):
            here = aligned(start, size)
            gain = gain_ref[:, here]
            ours = xin[j, :, here].astype(jnp.float32)
            theirs = xmate[s, j, :, here].astype(jnp.float32)
            left = jnp.concatenate(
                [(ours * gain).astype(jnp.bfloat16), (theirs * gain).astype(jnp.bfloat16)], axis=0
            )
            for p in parts:
                cols = cols_of(units[s], p)
                part = jnp.dot(left, wbuf[here, cols], preferred_element_type=jnp.float32)
                if fresh:
                    acc[:, cols] = part
                else:
                    acc[:, cols] += part
            if 0 in parts:
                squares = [(1 + s, theirs)] + ([(0, ours)] if s == 0 else [])
                for k, x in squares:
                    if fresh:
                        ssq[k] = fold(x * x)
                    else:
                        ssq[k] += fold(x * x)

        chip_rows = 2 * shard

        def arrive(i, p):
            for s in range(2):
                if i == 0:
                    swap(s, p).wait_recv()
                    circle(s, 1, 1, p).start()
                else:
                    k, b = (i + 1) // 2, (i + 1) % 2
                    circle(s, k, b, p).wait_recv()
                    if k < length - 1:
                        circle(s, k + 1, b, p).start()
                hand(s, i, p).start()

        def finish(i, p):
            for s in range(2):
                hand(s, i, p).wait_recv()

            @pl.when(sec == 0)
            def _():
                for s in range(2):
                    start = lax.div(owner_of(s, i), 2) * chip_rows
                    project(0, s, start, chip_rows, (p,), False)

        def drop(j):
            @pl.when(sec == 1 + j)
            def _():
                for c in range(chunks):
                    for s in range(2):
                        hand_on(s, j, c).wait_recv()
                        fall(s, j, c).start()

        drop(0)
        for p in range(PARTS):
            arrive(0, p)
        for p, s in both:
            stay(s, p).wait()
            mine(s, p).wait_recv()

        @pl.when(sec == 0)
        def _():
            for c in range(chunks):
                for s in range(2):
                    share(s, 0, c).wait_recv()
            for s in range(2):
                project(0, s, chip * chip_rows, chip_rows, range(PARTS), True)

        for p in range(PARTS):
            finish(0, p)
        for j in range(1, micro):
            drop(j)
        for i in range(1, waves):
            for p in range(PARTS):
                arrive(i, p)
                if p > 0:
                    finish(i, p - 1)
            finish(i, PARTS - 1)

        for j in range(micro):
            @pl.when(sec == 1 + j)
            def _():
                for c in range(chunks):
                    for s in range(2):
                        hand_on(s, j, c).wait_send()

        for s in range(2):
            tell(s).wait_recv()
        o_copy.wait()

        def ready(turn, region, unit, scale, heads):
            rows = slice(region * seq, (region + 1) * seq)
            for part, gains in ((0, qg_ref), (1, kg_ref)):
                factor = HEAD_DIM ** (-0.5) * LOG2_E if part == 0 else 1.0
                for i in heads:
                    start = unit * quarter + i * HEAD_DIM
                    p = acc[rows, aligned(part * model + start, HEAD_DIM)]
                    spot = (turn * 2 + part) * quarter + i * HEAD_DIM
                    qkv[:, spot : spot + HEAD_DIM] = lifted_norm(
                        p, scale, gains[:, aligned(start, HEAD_DIM)] * factor
                    )

        def attend(turn, region, unit, scale, allowed, heads, ref, base):
            ready(turn, region, unit, scale, heads)
            rows = slice(region * seq, (region + 1) * seq)
            for i in heads:
                spot = turn * 2 * quarter + i * HEAD_DIM
                v = acc[rows, aligned(2 * model + unit * quarter + i * HEAD_DIM, HEAD_DIM)] * scale
                ref[:, aligned(base + i * HEAD_DIM, HEAD_DIM)] = head(
                    qkv[:, spot : spot + HEAD_DIM],
                    qkv[:, spot + quarter : spot + quarter + HEAD_DIM], v, allowed,
                )

        def pass_on(j, c):
            hop(j, c).wait_recv()
            for s in range(2):
                share(s, j, c).start()

        @pl.loop(0, micro)
        def _(j):
            def ahead_of(n):
                for where, counts in ((sec == 1, EARLY[0]), (sec > 1, EARLY[1])):
                    if counts[n] > 0:
                        @pl.when(where & (j < micro - 1))
                        def _():
                            for c in range(sum(counts[:n]), sum(counts[: n + 1])):
                                pass_on(j + 1, c)

            @pl.when((sec > 0) | (j > 0))
            def _():
                def finish(g):
                    for c in range(g, g + GROUP):
                        for s in range(2):
                            share(s, j, c).wait_recv()
                    for s in range(2):
                        project(j, s, g * width, GROUP * width, range(PARTS), g == 0)

                for c in range(chunks + LAG):
                    if c < chunks:
                        late = ((sec == 1) & (c >= sum(EARLY[0]))) | ((sec > 1) & (c >= sum(EARLY[1])))

                        @pl.when((sec > 0) & ((j == 0) | late))
                        def _():
                            pass_on(j, c)

                    if c == chunks + LAG - 1:
                        ahead_of(0)
                    done = c - LAG + 1
                    if done > 0 and done % GROUP == 0:
                        finish(done - GROUP)

            def scale_of(k):
                square = jnp.sum(ssq[k], axis=-1, keepdims=True)
                return lax.rsqrt(square * (1.0 / model) + EPS)

            scales = [scale_of(1 + s) for s in range(2)]
            open_to = [
                mask(mate_spans[s, j, 0, 0:1, :], mate_spans[s, j, 1, 0:1, :]) for s in range(2)
            ]
            for n in range(RETURNS):
                heads = range(n * few // RETURNS, (n + 1) * few // RETURNS)
                for s in range(2):
                    attend(s, 1, units[s], scales[s], open_to[s], heads, ret.at[s, j], 0)
                for s in range(2):
                    give(s, j, n).start()

            ahead_of(1)
            which = order_ref[0, j]
            s0 = start_ref[0, which]
            allowed = mask(s0, s0 + len_ref[0, which])
            scale = scale_of(0)
            for s in range(2):
                attend(2 + s, 0, units[s], scale, allowed, range(few), att.at[j], units[s] * quarter)
            ahead_of(2)
            for n in range(RETURNS):
                for s in range(2):
                    give(s, j, n).wait_recv()
            ahead_of(3)
            leave(j)

        for s in range(2):
            tell(s).wait_send()
            for p in range(PARTS):
                swap(s, p).wait_send()
                mine(s, p).wait_send()
                for i in range(waves):
                    hand(s, i, p).wait_send()
                for k in range(1, length):
                    for b in range(2):
                        circle(s, k, b, p).wait_send()
            for j in range(micro):
                for n in range(RETURNS):
                    give(s, j, n).wait_send()

        @pl.when(sec > 0)
        def _():
            for s in range(2):
                for j in range(micro):
                    for c in range(chunks):
                        share(s, j, c).wait_send()

        for j in range(micro):
            @pl.when(sec == 1 + j)
            def _():
                for s in range(2):
                    for c in range(chunks):
                        fall(s, j, c).wait_send()

    @pl.when(jnp.logical_not(shared))
    def _():
        def rows(owner, way, sub):
            return pl.ds(pl.multiple_of(owner * shard + (way * SUBS + sub) * piece, piece), piece)

        def ring_copy(way, sub, step):
            owner = at(-step if way == 0 else step)
            where = rows(owner, way, sub)
            if step == 0:
                source = w_ref.at[pl.ds((way * SUBS + sub) * piece, piece)]
            else:
                source = wbuf.at[where]
            return pltpu.make_async_remote_copy(
                src_ref=source, dst_ref=wbuf.at[where],
                send_sem=ring_send.at[way, sub, step], recv_sem=ring_recv.at[way, sub, step],
                device_id=(sec, ahead if way == 0 else behind), device_id_type=MESH,
            )

        def pair_copy(way, sub, step):
            owner = at(-step if way == 0 else step)
            where = rows(owner, way, sub)
            return pltpu.make_async_remote_copy(
                src_ref=wbuf.at[where], dst_ref=wbuf.at[where],
                send_sem=pair_send.at[way, sub, step - 1], recv_sem=pair_recv.at[way, sub, step - 1],
                device_id=(sec, partner), device_id_type=MESH,
            )

        ring = {}
        pair = {}
        for sub in range(SUBS):
            for way in range(2):
                ring[way, sub, 0] = ring_copy(way, sub, 0)
                ring[way, sub, 0].start()
        first = pltpu.make_async_remote_copy(
            src_ref=w_ref, dst_ref=wbuf.at[own_rows], send_sem=first_send, recv_sem=first_recv,
            device_id=(sec, partner), device_id_type=MESH,
        )
        first.start()
        own.wait()
        first.wait_recv()
        for step in range(1, chips):
            for sub in range(SUBS):
                for way in range(2):
                    ring[way, sub, step - 1].wait_recv()
                    if step < chips - 1:
                        ring[way, sub, step] = ring_copy(way, sub, step)
                        ring[way, sub, step].start()
                    pair[way, sub, step] = pair_copy(way, sub, step)
                    pair[way, sub, step].start()
            for way in range(2):
                for sub in range(SUBS):
                    pair[way, sub, step].wait_recv()
        o_copy.wait()
        first.wait_send()
        for step in range(1, chips):
            for sub in range(SUBS):
                for way in range(2):
                    pair[way, sub, step].wait_send()
                    ring[way, sub, step - 1].wait_send()

        @pl.loop(0, micro)
        def _(j):
            which = order_ref[0, j]
            s0 = start_ref[0, which]
            s1 = s0 + len_ref[0, which]
            here_rows = slice(0, seq)
            square = jnp.zeros((seq, 1), jnp.float32)
            for g in range(0, chunks, GROUP):
                span = slice(g * width, (g + GROUP) * width)
                for c in range(g, g + GROUP):
                    hop(j, c).wait_recv()
                wide = xin[j, :, span].astype(jnp.float32)
                square = square + jnp.sum(wide * wide, axis=-1, keepdims=True)
                scaled = (wide * gain_ref[:, span]).astype(jnp.bfloat16)
                part = jnp.dot(scaled, wbuf[span, :], preferred_element_type=jnp.float32)
                if g == 0:
                    acc[here_rows, :] = part
                else:
                    acc[here_rows, :] += part

            scale = lax.rsqrt(square * (1.0 / model) + EPS)

            for part, gains in ((0, qg_ref), (1, kg_ref)):
                factor = HEAD_DIM ** (-0.5) * LOG2_E if part == 0 else 1.0

                @pl.loop(0, model // (NORMS_AT_ONCE * HEAD_DIM))
                def _(n):
                    for i in range(NORMS_AT_ONCE):
                        base = (n * NORMS_AT_ONCE + i) * HEAD_DIM
                        here = pl.ds(pl.multiple_of(base, HEAD_DIM), HEAD_DIM)
                        cols = pl.ds(pl.multiple_of(part * model + base, HEAD_DIM), HEAD_DIM)
                        qkv[:, cols] = lifted_norm(acc[here_rows, cols], scale, gains[:, here] * factor)

            allowed = mask(s0, s1)

            @pl.loop(0, model // (HEADS_AT_ONCE * HEAD_DIM))
            def _(n):
                for i in range(HEADS_AT_ONCE):
                    base = (n * HEADS_AT_ONCE + i) * HEAD_DIM
                    here = pl.ds(pl.multiple_of(base, HEAD_DIM), HEAD_DIM)
                    q = qkv[:, here]
                    k = qkv[:, pl.ds(pl.multiple_of(model + base, HEAD_DIM), HEAD_DIM)]
                    v = acc[here_rows, pl.ds(pl.multiple_of(2 * model + base, HEAD_DIM), HEAD_DIM)] * scale
                    att[j, :, here] = head(q, k, v, allowed)

            leave(j)

    for j in range(micro):
        for g in range(0, chunks, GROUP):
            out(j, g).wait()

    @pl.when(sec < sections - 1)
    def _():
        for j in range(micro):
            for c in range(chunks):
                hop(j, c).wait_send()


def solution(mesh):
    sections, devices = mesh.shape["section"], mesh.shape["dp"]

    def body(inputs, order, image_start, image_len, norm_gain, qkv_weight, q_gain, k_gain, o_weight):
        micro = order.shape[1]
        count, model = inputs.shape
        seq = count // micro
        total = qkv_weight.shape[2]
        shard = qkv_weight.shape[1]
        chunks = CHUNKS
        chips = devices // 2
        length = chips // 2
        smem = pl.BlockSpec(memory_space=pltpu.SMEM)
        vmem = pl.BlockSpec(memory_space=pltpu.VMEM)
        hbm = pl.BlockSpec(memory_space=pltpu.HBM)
        dma = pltpu.SemaphoreType.DMA
        out = pl.pallas_call(
            functools.partial(kernel, sections, devices),
            out_shape=jax.ShapeDtypeStruct((micro, seq, model), jnp.bfloat16),
            in_specs=[smem, smem, smem, vmem, vmem, hbm, vmem, vmem, hbm],
            out_specs=hbm,
            scratch_shapes=[
                pltpu.VMEM((model, total), jnp.bfloat16),
                pltpu.VMEM((model, model), jnp.bfloat16),
                pltpu.VMEM((micro, seq, model), jnp.bfloat16),
                pltpu.VMEM((micro, seq, model), jnp.bfloat16),
                pltpu.VMEM((2 * seq, total), jnp.float32),
                pltpu.VMEM((seq, 2 * model), jnp.bfloat16),
                pltpu.VMEM((micro, seq, model), jnp.bfloat16),
                pltpu.VMEM((2, micro, seq, model), jnp.bfloat16),
                pltpu.VMEM((2, micro, seq, model), jnp.bfloat16),
                pltpu.VMEM((2, micro, seq, model // 4), jnp.bfloat16),
                pltpu.VMEM((3, seq, 128), jnp.float32),
                pltpu.VMEM((micro, 2, 8, 128), jnp.int32),
                pltpu.VMEM((2, micro, 2, 8, 128), jnp.int32),
                dma, dma, dma, dma,
                dma((2, SUBS, chips - 1)),
                dma((2, SUBS, chips - 1)),
                dma((2, SUBS, chips - 1)),
                dma((2, SUBS, chips - 1)),
                dma((micro, chunks)),
                dma((micro, chunks)),
                dma((2, PARTS)),
                dma((2, PARTS)),
                dma((2, PARTS)),
                dma((2, length - 1, 2, PARTS)),
                dma((2, length - 1, 2, PARTS)),
                dma((2, 2 * length - 1, PARTS)),
                dma((2, 2 * length - 1, PARTS)),
                dma((2, PARTS)),
                dma((2, PARTS)),
                dma((2, micro, chunks)),
                dma((2, micro, chunks)),
                dma((2, micro, RETURNS)),
                dma((2, micro, RETURNS)),
                dma((2,)),
                dma((2,)),
                dma((2, micro, CHUNKS)),
                dma((2, micro, CHUNKS)),
                dma((2, micro, CHUNKS)),
                dma((micro, CHUNKS // GROUP)),
            ],
            compiler_params=pltpu.CompilerParams(
                collective_id=0, has_side_effects=True, vmem_limit_bytes=60 * 1024 * 1024
            ),
        )(
            order, image_start, image_len, inputs.reshape(micro, seq, model), norm_gain,
            qkv_weight.reshape(shard, total), q_gain, k_gain, o_weight.reshape(model, model),
        )
        return out.reshape(1, count, model)

    in_specs = (
        P("dp", None),
        P("dp", None),
        P("dp", None),
        P("dp", None),
        P("section", None),
        P("section", "dp", None),
        P("section", None),
        P("section", None),
        P("section", None, None),
    )
    out_specs = P("section", "dp", None)
    return jax.shard_map(body, mesh=mesh, in_specs=in_specs, out_specs=out_specs, check_vma=False)
```

```python
import functools
import jax
import jax.numpy as jnp
from jax import lax
from jax.experimental import pallas as pl
from jax.experimental.pallas import tpu as pltpu
from jax.sharding import PartitionSpec as P

HEAD_DIM = 128
EPS = 1e-05
LOG2_E = 1.4426950408889634
SUBS = 2
CHUNKS = 8
GROUP = 2
LAG = 5
EARLY = ((2, 2, 1, 1, 1), (0, 2, 1, 1, 1))
CARRIER = 2
CARRIED = 2
HEADS_AT_ONCE = 16
NORMS_AT_ONCE = 16
SHARED_SECTIONS = 3
PARTS = 3
RETURNS = 2
MESH = pl.DeviceIdType.MESH


def grid_of(chips):
    columns = 1
    while columns * columns < chips:
        columns *= 2
    return chips // columns, columns


def ring_order(chips):
    rows, columns = grid_of(chips)
    cells = []
    for r in range(rows):
        line = list(range(1, columns))
        cells += [r * columns + c for c in (line if r % 2 == 0 else line[::-1])]
    cells += [r * columns for r in reversed(range(rows))]
    return cells


def look(table, index):
    found = jnp.int32(0)
    for i, value in enumerate(table):
        found = found + jnp.where(index == i, jnp.int32(value), jnp.int32(0))
    return found


def flip(value):
    return value + 1 - 2 * lax.rem(value, 2)


def aligned(start, size):
    return pl.ds(start if isinstance(start, int) else pl.multiple_of(start, size), size)


def kernel(
    sections, devices,
    order_ref, start_ref, len_ref, x_ref, gain_ref, w_ref, qg_ref, kg_ref, o_ref,
    out_ref,
    wbuf, obuf, xin, xout, acc, qkv, att, xmate, relay, ret, ssq, spans, mate_spans, wup, wover,
    own_sem, o_sem, first_send, first_recv, ring_send, ring_recv, pair_send, pair_recv,
    hop_send, hop_recv,
    own_sems, swap_send, swap_recv, loop_send, loop_recv, core_send, core_recv,
    mine_send, mine_recv, x_send, x_recv, give_send, give_recv, span_send, span_recv,
    pass_send, pass_recv, fall_send, out_sem,
    up_send, up_recv, over_send, over_recv, down_send,
):
    chips = devices // 2
    grid_rows, columns = grid_of(chips)
    order = ring_order(chips)
    inverse = [order.index(c) for c in range(chips)]
    shard, total = w_ref.shape
    piece = shard // (2 * SUBS)
    micro, seq, model = xin.shape
    chunks, width = CHUNKS, model // CHUNKS
    quarter = model // 4
    few = quarter // HEAD_DIM
    sec = lax.axis_index("section")
    me = lax.axis_index("dp")
    core = lax.rem(me, 2)
    chip = lax.div(me, 2)
    place = look(inverse, chip)
    partner = flip(me)

    def at(offset):
        return look(order, lax.rem(place + (offset % chips), chips)) * 2 + core

    ahead, behind = at(1), at(-1)
    above = lax.rem(sec + 1, sections)
    below = lax.rem(sec + sections - 1, sections)

    row, col = lax.div(chip, columns), lax.rem(chip, columns)
    across, down = lax.rem(col, 2), lax.rem(row, 2)
    units = (across, 2 + down)
    half_c, half_r = columns // 2, grid_rows // 2
    places = (row * half_c + lax.div(col, 2), col * half_r + lax.div(row, 2))
    length = chips // 2

    def device(r, c):
        return (r * columns + c) * 2 + core

    mates = (device(row, flip(col)), device(flip(row), col))

    def seat(s, offset, mate):
        spot = lax.rem(places[s] + (offset % length), length)
        if s == 0:
            r, c = lax.div(spot, half_c), 2 * lax.rem(spot, half_c) + across
            c = flip(c) if mate else c
        else:
            c, r = lax.div(spot, half_r), 2 * lax.rem(spot, half_r) + down
            r = flip(r) if mate else r
        return device(r, c)

    def block(owner):
        return aligned(owner * shard, shard)

    def cols_of(unit, part):
        return aligned(part * model + unit * quarter, quarter)

    shared = sec < SHARED_SECTIONS

    def stay(s, p):
        where = cols_of(units[s], p)
        return pltpu.make_async_copy(w_ref.at[:, where], wbuf.at[block(me), where], own_sems.at[s, p])

    relays = [3 - j for j in range(micro)]
    edges = sorted({(0, r) for r in relays} | {(0, CARRIER), (CARRIER, 0)})
    barrier = pltpu.get_barrier_semaphore()
    near = [mates[0], mates[1], partner]
    if chips > 4:
        near += [ahead, behind]
        for s in range(2):
            near += [seat(s, 1, False), seat(s, -1, False)]
    for other in near:
        pl.semaphore_signal(barrier, inc=1, device_id=(sec, other), device_id_type=MESH)
    line = (sec < sections - 1).astype(jnp.int32)
    for source, target in edges:
        @pl.when(sec == source)
        def _():
            pl.semaphore_signal(barrier, inc=1, device_id=(target, me), device_id_type=MESH)

        line = line + (sec == target).astype(jnp.int32)

    @pl.when(sec > 0)
    def _():
        pl.semaphore_signal(barrier, inc=1, device_id=(below, me), device_id_type=MESH)

    o_copy = pltpu.make_async_copy(o_ref, obuf, o_sem)
    own_rows = block(me)
    own = pltpu.make_async_copy(w_ref, wbuf.at[own_rows], own_sem)

    @pl.when(shared)
    def _():
        for s in range(2):
            for p in range(PARTS):
                stay(s, p).start()
        for j in range(micro):
            which = order_ref[0, j]
            s0 = start_ref[0, which]
            spans[j, 0] = jnp.full(spans.shape[2:], s0, jnp.int32)
            spans[j, 1] = jnp.full(spans.shape[2:], s0 + len_ref[0, which], jnp.int32)

            @pl.when(sec == 0)
            def _():
                xin[j] = x_ref[which]

    for j in range(micro):
        @pl.when(sec == relays[j])
        def _():
            xout[j] = x_ref[order_ref[0, j]]

    @pl.when(jnp.logical_not(shared))
    def _():
        own.start()

    o_copy.start()

    pl.semaphore_wait(barrier, len(near) + line)

    def span_of(c):
        return pl.ds(c * width, width)

    def hop(j, c):
        return pltpu.make_async_remote_copy(
            src_ref=xout.at[j, :, span_of(c)], dst_ref=xin.at[j, :, span_of(c)],
            send_sem=hop_send.at[j, c], recv_sem=hop_recv.at[j, c],
            device_id=(above, me), device_id_type=MESH,
        )

    row_id = lax.broadcasted_iota(jnp.int32, (seq, seq), 0)
    col_id = lax.broadcasted_iota(jnp.int32, (seq, seq), 1)

    def mask(s0, s1):
        return (col_id <= row_id) | (
            (row_id >= s0) & (row_id < s1) & (col_id >= s0) & (col_id < s1)
        )

    def remote(source, dest, sent, got, other, level=None):
        return pltpu.make_async_remote_copy(
            src_ref=source, dst_ref=dest, send_sem=sent, recv_sem=got,
            device_id=(sec if level is None else level, other), device_id_type=MESH,
        )

    def hand_on(s, j, c):
        return remote(
            xout.at[j, :, span_of(c)], relay.at[s, j, :, span_of(c)],
            pass_send.at[s, j, c], pass_recv.at[s, j, c], mates[s],
        )

    def fall(s, j, c):
        return remote(
            relay.at[s, j, :, span_of(c)], xmate.at[s, j, :, span_of(c)],
            fall_send.at[s, j, c], x_recv.at[s, j, c], me, 0,
        )

    pieces = [(c, s) for c in range(chunks) for s in range(2)]

    def lift(j):
        @pl.when(sec == relays[j])
        def _():
            for c, s in pieces:
                hand_on(s, j, c).start()

    def drop(j):
        @pl.when(sec == relays[j])
        def _():
            for c, s in pieces:
                hand_on(s, j, c).wait_recv()
                fall(s, j, c).start()
            for c, s in pieces:
                hand_on(s, j, c).wait_send()

    low = [j for j in range(micro) if relays[j] < SHARED_SECTIONS]
    high = [j for j in range(micro) if relays[j] >= SHARED_SECTIONS]

    def out(j, g):
        here = (j, slice(None), pl.ds(g * width, GROUP * width))
        return pltpu.make_async_copy(xout.at[here], out_ref.at[here], out_sem.at[j, g // GROUP])

    def leave(j, between=None):
        for g in range(0, chunks, GROUP):
            if between is not None and g == chunks // 2:
                between()
            span = slice(g * width, (g + GROUP) * width)
            grown = jnp.dot(att[j], obuf[:, span], preferred_element_type=jnp.float32)
            fresh = (xin[j, :, span].astype(jnp.float32) + grown).astype(jnp.bfloat16)
            xout[j, :, span] = fresh
            out(j, g).start()

            @pl.when(sec < sections - 1)
            def _():
                for c in range(g, g + GROUP):
                    hop(j, c).start()

    def head(q, k, v, allowed):
        scores = lax.dot_general(
            q, k, (((1,), (1,)), ((), ())), preferred_element_type=jnp.float32
        )
        lifted = jnp.where(allowed, jnp.exp2(scores), 0.0)
        mixed = jnp.dot(
            lifted.astype(jnp.bfloat16), v.astype(jnp.bfloat16),
            preferred_element_type=jnp.float32,
        )
        return (mixed * (1.0 / jnp.sum(lifted, axis=-1, keepdims=True))).astype(jnp.bfloat16)

    def lifted_norm(p, scale, gain):
        mean = jnp.mean(p * p, axis=-1, keepdims=True) * scale * scale
        return (p * (lax.rsqrt(mean + EPS) * scale) * gain).astype(jnp.bfloat16)

    @pl.when(shared)
    def _():
        def swap(s, p):
            where = cols_of(flip(units[s]), p)
            return remote(
                w_ref.at[:, where], wbuf.at[own_rows, where],
                swap_send.at[s, p], swap_recv.at[s, p], mates[s],
            )

        def circle(s, k, b, p):
            where = cols_of(units[s], p)
            rows = block(seat(s, 1 - k, b == 1))
            source = w_ref.at[:, where] if k == 1 and b == 0 else wbuf.at[rows, where]
            return remote(
                source, wbuf.at[rows, where],
                loop_send.at[s, k - 1, b, p], loop_recv.at[s, k - 1, b, p], seat(s, 1, False),
            )

        def owner_of(s, i):
            return mates[s] if i == 0 else seat(s, -((i + 1) // 2), i % 2 == 0)

        def hand(s, i, p):
            here = wbuf.at[block(owner_of(s, i)), cols_of(units[s], p)]
            return remote(here, here, core_send.at[s, i, p], core_recv.at[s, i, p], partner)

        def mine(s, p):
            where = cols_of(units[s], p)
            return remote(
                w_ref.at[:, where], wbuf.at[own_rows, where],
                mine_send.at[s, p], mine_recv.at[s, p], partner,
            )

        def share(s, j, c):
            return remote(
                xin.at[j, :, span_of(c)], xmate.at[s, j, :, span_of(c)],
                x_send.at[s, j, c], x_recv.at[s, j, c], mates[s],
            )

        lot = quarter // RETURNS

        def give(s, j, n):
            return remote(
                ret.at[s, j, :, pl.ds(n * lot, lot)],
                att.at[j, :, aligned(units[s] * quarter + n * lot, lot)],
                give_send.at[s, j, n], give_recv.at[s, j, n], mates[s],
            )

        def tell(s):
            return remote(spans, mate_spans.at[s], span_send.at[s], span_recv.at[s], mates[s])

        both = [(p, s) for p in range(PARTS) for s in range(2)]
        waves = 2 * length - 1

        for s in range(2):
            tell(s).start()

        def climb(s):
            return remote(
                w_ref.at[:, cols_of(units[s], CARRIED)], wup.at[s],
                up_send.at[s], up_recv.at[s], me, CARRIER,
            )

        def cross(s):
            return remote(
                wup.at[s], wover.at[s], over_send.at[s], over_recv.at[s], seat(s, 1, False)
            )

        def sink(s):
            rows = block(seat(s, -1, False))
            return remote(
                wover.at[s], wbuf.at[rows, cols_of(units[s], CARRIED)],
                down_send.at[s], loop_recv.at[s, 0, 0, CARRIED], me, 0,
            )

        @pl.when(sec == 0)
        def _():
            for s in range(2):
                climb(s).start()

        for p, s in both[:4]:
            swap(s, p).start()
        for p, s in both:
            mine(s, p).start()

        @pl.when(sec == CARRIER)
        def _():
            for s in range(2):
                climb(s).wait_recv()
                cross(s).start()

        for j in low:
            lift(j)
        for p, s in both[4:]:
            swap(s, p).start()
        for p, s in both:
            if p == CARRIED:
                @pl.when(sec > 0)
                def _():
                    circle(s, 1, 0, p).start()
            else:
                circle(s, 1, 0, p).start()

        def fold(x):
            out = x[:, :128]
            for i in range(1, x.shape[1] // 128):
                out = out + x[:, i * 128 : (i + 1) * 128]
            return out

        def project(j, s, start, size, parts, fresh):
            here = aligned(start, size)
            gain = gain_ref[:, here]
            ours = xin[j, :, here].astype(jnp.float32)
            theirs = xmate[s, j, :, here].astype(jnp.float32)
            left = jnp.concatenate(
                [(ours * gain).astype(jnp.bfloat16), (theirs * gain).astype(jnp.bfloat16)], axis=0
            )
            for p in parts:
                cols = cols_of(units[s], p)
                part = jnp.dot(left, wbuf[here, cols], preferred_element_type=jnp.float32)
                if fresh:
                    acc[:, cols] = part
                else:
                    acc[:, cols] += part
            if 0 in parts:
                squares = [(1 + s, theirs)] + ([(0, ours)] if s == 0 else [])
                for k, x in squares:
                    if fresh:
                        ssq[k] = fold(x * x)
                    else:
                        ssq[k] += fold(x * x)

        chip_rows = 2 * shard

        def arrive(i, p):
            for s in range(2):
                if i == 0:
                    swap(s, p).wait_recv()
                    circle(s, 1, 1, p).start()
                else:
                    k, b = (i + 1) // 2, (i + 1) % 2
                    circle(s, k, b, p).wait_recv()
                    if k < length - 1:
                        circle(s, k + 1, b, p).start()
                hand(s, i, p).start()

        def finish(i, p):
            for s in range(2):
                hand(s, i, p).wait_recv()

            @pl.when(sec == 0)
            def _():
                for s in range(2):
                    start = lax.div(owner_of(s, i), 2) * chip_rows
                    project(0, s, start, chip_rows, (p,), False)

        for p in range(PARTS - 1):
            arrive(0, p)

        @pl.when(sec == CARRIER)
        def _():
            for s in range(2):
                cross(s).wait_recv()
                sink(s).start()

        for j in low:
            drop(j)
        arrive(0, PARTS - 1)
        for p, s in both:
            stay(s, p).wait()
            mine(s, p).wait_recv()

        @pl.when(sec == 0)
        def _():
            for c in range(chunks):
                for s in range(2):
                    share(s, 0, c).wait_recv()
            for s in range(2):
                project(0, s, chip * chip_rows, chip_rows, range(PARTS), True)

        for p in range(PARTS):
            finish(0, p)
        for i in range(1, waves):
            for p in range(PARTS):
                arrive(i, p)
                if p > 0:
                    finish(i, p - 1)
            finish(i, PARTS - 1)

        for s in range(2):
            tell(s).wait_recv()
        o_copy.wait()

        def ready(turn, region, unit, scale, heads):
            rows = slice(region * seq, (region + 1) * seq)
            for part, gains in ((0, qg_ref), (1, kg_ref)):
                factor = HEAD_DIM ** (-0.5) * LOG2_E if part == 0 else 1.0
                for i in heads:
                    start = unit * quarter + i * HEAD_DIM
                    p = acc[rows, aligned(part * model + start, HEAD_DIM)]
                    spot = (turn * 2 + part) * quarter + i * HEAD_DIM
                    qkv[:, spot : spot + HEAD_DIM] = lifted_norm(
                        p, scale, gains[:, aligned(start, HEAD_DIM)] * factor
                    )

        def attend(turn, region, unit, scale, allowed, heads, ref, base):
            ready(turn, region, unit, scale, heads)
            rows = slice(region * seq, (region + 1) * seq)
            for i in heads:
                spot = turn * 2 * quarter + i * HEAD_DIM
                v = acc[rows, aligned(2 * model + unit * quarter + i * HEAD_DIM, HEAD_DIM)] * scale
                ref[:, aligned(base + i * HEAD_DIM, HEAD_DIM)] = head(
                    qkv[:, spot : spot + HEAD_DIM],
                    qkv[:, spot + quarter : spot + quarter + HEAD_DIM], v, allowed,
                )

        def pass_on(j, c):
            hop(j, c).wait_recv()
            for s in range(2):
                share(s, j, c).start()

        @pl.loop(0, micro)
        def _(j):
            def ahead_of(n):
                for where, counts in ((sec == 1, EARLY[0]), (sec > 1, EARLY[1])):
                    if counts[n] > 0:
                        @pl.when(where & (j < micro - 1))
                        def _():
                            for c in range(sum(counts[:n]), sum(counts[: n + 1])):
                                pass_on(j + 1, c)

            @pl.when((sec > 0) | (j > 0))
            def _():
                def finish(g):
                    for c in range(g, g + GROUP):
                        for s in range(2):
                            share(s, j, c).wait_recv()
                    for s in range(2):
                        project(j, s, g * width, GROUP * width, range(PARTS), g == 0)

                for c in range(chunks + LAG):
                    if c < chunks:
                        late = ((sec == 1) & (c >= sum(EARLY[0]))) | ((sec > 1) & (c >= sum(EARLY[1])))

                        @pl.when((sec > 0) & ((j == 0) | late))
                        def _():
                            pass_on(j, c)

                    if c == chunks + LAG - 1:
                        ahead_of(0)
                    done = c - LAG + 1
                    if done > 0 and done % GROUP == 0:
                        finish(done - GROUP)

            def scale_of(k):
                square = jnp.sum(ssq[k], axis=-1, keepdims=True)
                return lax.rsqrt(square * (1.0 / model) + EPS)

            scales = [scale_of(1 + s) for s in range(2)]
            open_to = [
                mask(mate_spans[s, j, 0, 0:1, :], mate_spans[s, j, 1, 0:1, :]) for s in range(2)
            ]
            for n in range(RETURNS):
                heads = range(n * few // RETURNS, (n + 1) * few // RETURNS)
                for s in range(2):
                    attend(s, 1, units[s], scales[s], open_to[s], heads, ret.at[s, j], 0)
                for s in range(2):
                    give(s, j, n).start()

            ahead_of(1)
            which = order_ref[0, j]
            s0 = start_ref[0, which]
            allowed = mask(s0, s0 + len_ref[0, which])
            scale = scale_of(0)
            for s in range(2):
                attend(2 + s, 0, units[s], scale, allowed, range(few), att.at[j], units[s] * quarter)
            ahead_of(2)
            for n in range(RETURNS):
                for s in range(2):
                    give(s, j, n).wait_recv()
            ahead_of(3)
            leave(j, lambda: ahead_of(4))

        for s in range(2):
            tell(s).wait_send()
            for p in range(PARTS):
                swap(s, p).wait_send()
                mine(s, p).wait_send()
                for i in range(waves):
                    hand(s, i, p).wait_send()
                for k in range(1, length):
                    for b in range(2):
                        if (k, b, p) != (1, 0, CARRIED):
                            circle(s, k, b, p).wait_send()
            for j in range(micro):
                for n in range(RETURNS):
                    give(s, j, n).wait_send()

        @pl.when(sec > 0)
        def _():
            for s in range(2):
                circle(s, 1, 0, CARRIED).wait_send()
                for j in range(micro):
                    for c in range(chunks):
                        share(s, j, c).wait_send()

        @pl.when(sec == 0)
        def _():
            for s in range(2):
                climb(s).wait_send()

        @pl.when(sec == CARRIER)
        def _():
            for s in range(2):
                cross(s).wait_send()
                sink(s).wait_send()

    @pl.when(jnp.logical_not(shared))
    def _():
        def rows(owner, way, sub):
            return pl.ds(pl.multiple_of(owner * shard + (way * SUBS + sub) * piece, piece), piece)

        def ring_copy(way, sub, step):
            owner = at(-step if way == 0 else step)
            where = rows(owner, way, sub)
            if step == 0:
                source = w_ref.at[pl.ds((way * SUBS + sub) * piece, piece)]
            else:
                source = wbuf.at[where]
            return pltpu.make_async_remote_copy(
                src_ref=source, dst_ref=wbuf.at[where],
                send_sem=ring_send.at[way, sub, step], recv_sem=ring_recv.at[way, sub, step],
                device_id=(sec, ahead if way == 0 else behind), device_id_type=MESH,
            )

        def pair_copy(way, sub, step):
            owner = at(-step if way == 0 else step)
            where = rows(owner, way, sub)
            return pltpu.make_async_remote_copy(
                src_ref=wbuf.at[where], dst_ref=wbuf.at[where],
                send_sem=pair_send.at[way, sub, step - 1], recv_sem=pair_recv.at[way, sub, step - 1],
                device_id=(sec, partner), device_id_type=MESH,
            )

        for j in high:
            lift(j)
        ring = {}
        pair = {}
        for sub in range(SUBS):
            for way in range(2):
                ring[way, sub, 0] = ring_copy(way, sub, 0)
                ring[way, sub, 0].start()
        first = pltpu.make_async_remote_copy(
            src_ref=w_ref, dst_ref=wbuf.at[own_rows], send_sem=first_send, recv_sem=first_recv,
            device_id=(sec, partner), device_id_type=MESH,
        )
        first.start()
        for j in high:
            drop(j)
        own.wait()
        first.wait_recv()
        for step in range(1, chips):
            for sub in range(SUBS):
                for way in range(2):
                    ring[way, sub, step - 1].wait_recv()
                    if step < chips - 1:
                        ring[way, sub, step] = ring_copy(way, sub, step)
                        ring[way, sub, step].start()
                    pair[way, sub, step] = pair_copy(way, sub, step)
                    pair[way, sub, step].start()
            for way in range(2):
                for sub in range(SUBS):
                    pair[way, sub, step].wait_recv()
        o_copy.wait()
        first.wait_send()
        for step in range(1, chips):
            for sub in range(SUBS):
                for way in range(2):
                    pair[way, sub, step].wait_send()
                    ring[way, sub, step - 1].wait_send()

        @pl.loop(0, micro)
        def _(j):
            which = order_ref[0, j]
            s0 = start_ref[0, which]
            s1 = s0 + len_ref[0, which]
            here_rows = slice(0, seq)
            square = jnp.zeros((seq, 1), jnp.float32)
            for g in range(0, chunks, GROUP):
                span = slice(g * width, (g + GROUP) * width)
                for c in range(g, g + GROUP):
                    hop(j, c).wait_recv()
                wide = xin[j, :, span].astype(jnp.float32)
                square = square + jnp.sum(wide * wide, axis=-1, keepdims=True)
                scaled = (wide * gain_ref[:, span]).astype(jnp.bfloat16)
                part = jnp.dot(scaled, wbuf[span, :], preferred_element_type=jnp.float32)
                if g == 0:
                    acc[here_rows, :] = part
                else:
                    acc[here_rows, :] += part

            scale = lax.rsqrt(square * (1.0 / model) + EPS)

            for part, gains in ((0, qg_ref), (1, kg_ref)):
                factor = HEAD_DIM ** (-0.5) * LOG2_E if part == 0 else 1.0

                @pl.loop(0, model // (NORMS_AT_ONCE * HEAD_DIM))
                def _(n):
                    for i in range(NORMS_AT_ONCE):
                        base = (n * NORMS_AT_ONCE + i) * HEAD_DIM
                        here = pl.ds(pl.multiple_of(base, HEAD_DIM), HEAD_DIM)
                        cols = pl.ds(pl.multiple_of(part * model + base, HEAD_DIM), HEAD_DIM)
                        qkv[:, cols] = lifted_norm(acc[here_rows, cols], scale, gains[:, here] * factor)

            allowed = mask(s0, s1)

            @pl.loop(0, model // (HEADS_AT_ONCE * HEAD_DIM))
            def _(n):
                for i in range(HEADS_AT_ONCE):
                    base = (n * HEADS_AT_ONCE + i) * HEAD_DIM
                    here = pl.ds(pl.multiple_of(base, HEAD_DIM), HEAD_DIM)
                    q = qkv[:, here]
                    k = qkv[:, pl.ds(pl.multiple_of(model + base, HEAD_DIM), HEAD_DIM)]
                    v = acc[here_rows, pl.ds(pl.multiple_of(2 * model + base, HEAD_DIM), HEAD_DIM)] * scale
                    att[j, :, here] = head(q, k, v, allowed)

            leave(j)

    for j in range(micro):
        for g in range(0, chunks, GROUP):
            out(j, g).wait()

        @pl.when(sec == relays[j])
        def _():
            for c, s in pieces:
                fall(s, j, c).wait_send()

    @pl.when(sec < sections - 1)
    def _():
        for j in range(micro):
            for c in range(chunks):
                hop(j, c).wait_send()


def solution(mesh):
    sections, devices = mesh.shape["section"], mesh.shape["dp"]

    def body(inputs, order, image_start, image_len, norm_gain, qkv_weight, q_gain, k_gain, o_weight):
        micro = order.shape[1]
        count, model = inputs.shape
        seq = count // micro
        total = qkv_weight.shape[2]
        shard = qkv_weight.shape[1]
        chunks = CHUNKS
        chips = devices // 2
        length = chips // 2
        smem = pl.BlockSpec(memory_space=pltpu.SMEM)
        vmem = pl.BlockSpec(memory_space=pltpu.VMEM)
        hbm = pl.BlockSpec(memory_space=pltpu.HBM)
        dma = pltpu.SemaphoreType.DMA
        out = pl.pallas_call(
            functools.partial(kernel, sections, devices),
            out_shape=jax.ShapeDtypeStruct((micro, seq, model), jnp.bfloat16),
            in_specs=[smem, smem, smem, vmem, vmem, hbm, vmem, vmem, hbm],
            out_specs=hbm,
            scratch_shapes=[
                pltpu.VMEM((model, total), jnp.bfloat16),
                pltpu.VMEM((model, model), jnp.bfloat16),
                pltpu.VMEM((micro, seq, model), jnp.bfloat16),
                pltpu.VMEM((micro, seq, model), jnp.bfloat16),
                pltpu.VMEM((2 * seq, total), jnp.float32),
                pltpu.VMEM((seq, 2 * model), jnp.bfloat16),
                pltpu.VMEM((micro, seq, model), jnp.bfloat16),
                pltpu.VMEM((2, micro, seq, model), jnp.bfloat16),
                pltpu.VMEM((2, micro, seq, model), jnp.bfloat16),
                pltpu.VMEM((2, micro, seq, model // 4), jnp.bfloat16),
                pltpu.VMEM((3, seq, 128), jnp.float32),
                pltpu.VMEM((micro, 2, 8, 128), jnp.int32),
                pltpu.VMEM((2, micro, 2, 8, 128), jnp.int32),
                pltpu.VMEM((2, shard, model // 4), jnp.bfloat16),
                pltpu.VMEM((2, shard, model // 4), jnp.bfloat16),
                dma, dma, dma, dma,
                dma((2, SUBS, chips - 1)),
                dma((2, SUBS, chips - 1)),
                dma((2, SUBS, chips - 1)),
                dma((2, SUBS, chips - 1)),
                dma((micro, chunks)),
                dma((micro, chunks)),
                dma((2, PARTS)),
                dma((2, PARTS)),
                dma((2, PARTS)),
                dma((2, length - 1, 2, PARTS)),
                dma((2, length - 1, 2, PARTS)),
                dma((2, 2 * length - 1, PARTS)),
                dma((2, 2 * length - 1, PARTS)),
                dma((2, PARTS)),
                dma((2, PARTS)),
                dma((2, micro, chunks)),
                dma((2, micro, chunks)),
                dma((2, micro, RETURNS)),
                dma((2, micro, RETURNS)),
                dma((2,)),
                dma((2,)),
                dma((2, micro, CHUNKS)),
                dma((2, micro, CHUNKS)),
                dma((2, micro, CHUNKS)),
                dma((micro, CHUNKS // GROUP)),
                dma((2,)),
                dma((2,)),
                dma((2,)),
                dma((2,)),
                dma((2,)),
            ],
            compiler_params=pltpu.CompilerParams(
                collective_id=0, has_side_effects=True, vmem_limit_bytes=60 * 1024 * 1024
            ),
        )(
            order, image_start, image_len, inputs.reshape(micro, seq, model), norm_gain,
            qkv_weight.reshape(shard, total), q_gain, k_gain, o_weight.reshape(model, model),
        )
        return out.reshape(1, count, model)

    in_specs = (
        P("dp", None),
        P("dp", None),
        P("dp", None),
        P("dp", None),
        P("section", None),
        P("section", "dp", None),
        P("section", None),
        P("section", None),
        P("section", None, None),
    )
    out_specs = P("section", "dp", None)
    return jax.shard_map(body, mesh=mesh, in_specs=in_specs, out_specs=out_specs, check_vma=False)
```

```python
import functools
import jax
import jax.numpy as jnp
from jax import lax
from jax.experimental import pallas as pl
from jax.experimental.pallas import tpu as pltpu
from jax.sharding import PartitionSpec as P

HEAD_DIM = 128
EPS = 1e-05
LOG2_E = 1.4426950408889634
SUBS = 2
CHUNKS = 8
GROUPS = (2, 2, 2, 2)
EXITS = (2, 2, 2, 2)
LAG = 5
EARLY = ((2, 2, 1, 1, 1), (0, 2, 1, 1, 1))
CARRIER = 2
CARRIED = 2
HEADS_AT_ONCE = 16
NORMS_AT_ONCE = 16
SHARED_SECTIONS = 3
PARTS = 3
RETURNS = 2
MESH = pl.DeviceIdType.MESH


def grid_of(chips):
    columns = 1
    while columns * columns < chips:
        columns *= 2
    return chips // columns, columns


def ring_order(chips):
    rows, columns = grid_of(chips)
    cells = []
    for r in range(rows):
        line = list(range(1, columns))
        cells += [r * columns + c for c in (line if r % 2 == 0 else line[::-1])]
    cells += [r * columns for r in reversed(range(rows))]
    return cells


def look(table, index):
    found = jnp.int32(0)
    for i, value in enumerate(table):
        found = found + jnp.where(index == i, jnp.int32(value), jnp.int32(0))
    return found


def flip(value):
    return value + 1 - 2 * lax.rem(value, 2)


def runs(sizes):
    return [(sum(sizes[:n]), size) for n, size in enumerate(sizes)]


def aligned(start, size):
    return pl.ds(start if isinstance(start, int) else pl.multiple_of(start, size), size)


def kernel(
    sections, devices,
    order_ref, start_ref, len_ref, x_hbm, gain_ref, w_ref, qg_ref, kg_ref, o_ref,
    out_ref,
    wbuf, obuf, xin, xout, acc, qkv, att, xmate, relay, ret, ssq, spans, mate_spans, wup, wover,
    own_sem, o_sem, first_send, first_recv, ring_send, ring_recv, pair_send, pair_recv,
    hop_send, hop_recv,
    own_sems, swap_send, swap_recv, loop_send, loop_recv, core_send, core_recv,
    mine_send, mine_recv, x_send, x_recv, give_send, give_recv, span_send, span_recv,
    pass_send, pass_recv, fall_send, out_sem,
    up_send, up_recv, over_send, over_recv, down_send, x_ref, x_sem,
):
    chips = devices // 2
    grid_rows, columns = grid_of(chips)
    order = ring_order(chips)
    inverse = [order.index(c) for c in range(chips)]
    shard, total = w_ref.shape
    piece = shard // (2 * SUBS)
    micro, seq, model = xin.shape
    chunks, width = CHUNKS, model // CHUNKS
    quarter = model // 4
    few = quarter // HEAD_DIM
    sec = lax.axis_index("section")
    me = lax.axis_index("dp")
    core = lax.rem(me, 2)
    chip = lax.div(me, 2)
    place = look(inverse, chip)
    partner = flip(me)

    def at(offset):
        return look(order, lax.rem(place + (offset % chips), chips)) * 2 + core

    ahead, behind = at(1), at(-1)
    above = lax.rem(sec + 1, sections)
    below = lax.rem(sec + sections - 1, sections)

    row, col = lax.div(chip, columns), lax.rem(chip, columns)
    across, down = lax.rem(col, 2), lax.rem(row, 2)
    units = (across, 2 + down)
    half_c, half_r = columns // 2, grid_rows // 2
    places = (row * half_c + lax.div(col, 2), col * half_r + lax.div(row, 2))
    length = chips // 2

    def device(r, c):
        return (r * columns + c) * 2 + core

    mates = (device(row, flip(col)), device(flip(row), col))

    def seat(s, offset, mate):
        spot = lax.rem(places[s] + (offset % length), length)
        if s == 0:
            r, c = lax.div(spot, half_c), 2 * lax.rem(spot, half_c) + across
            c = flip(c) if mate else c
        else:
            c, r = lax.div(spot, half_r), 2 * lax.rem(spot, half_r) + down
            r = flip(r) if mate else r
        return device(r, c)

    def block(owner):
        return aligned(owner * shard, shard)

    def cols_of(unit, part):
        return aligned(part * model + unit * quarter, quarter)

    shared = sec < SHARED_SECTIONS

    def stay(s, p):
        where = cols_of(units[s], p)
        return pltpu.make_async_copy(w_ref.at[:, where], wbuf.at[block(me), where], own_sems.at[s, p])

    relays = [3 - j for j in range(micro)]
    edges = sorted({(0, r) for r in relays} | {(0, CARRIER), (CARRIER, 0)})
    x_copy = pltpu.make_async_copy(x_hbm, x_ref, x_sem)
    x_copy.start()
    barrier = pltpu.get_barrier_semaphore()
    near = [mates[0], mates[1], partner]
    if chips > 4:
        near += [ahead, behind]
        for s in range(2):
            near += [seat(s, 1, False), seat(s, -1, False)]
    for other in near:
        pl.semaphore_signal(barrier, inc=1, device_id=(sec, other), device_id_type=MESH)
    line = (sec < sections - 1).astype(jnp.int32)
    for source, target in edges:
        @pl.when(sec == source)
        def _():
            pl.semaphore_signal(barrier, inc=1, device_id=(target, me), device_id_type=MESH)

        line = line + (sec == target).astype(jnp.int32)

    @pl.when(sec > 0)
    def _():
        pl.semaphore_signal(barrier, inc=1, device_id=(below, me), device_id_type=MESH)

    o_copy = pltpu.make_async_copy(o_ref, obuf, o_sem)
    own_rows = block(me)
    own = pltpu.make_async_copy(w_ref, wbuf.at[own_rows], own_sem)

    @pl.when(shared)
    def _():
        for s in range(2):
            for p in range(PARTS):
                stay(s, p).start()

    x_copy.wait()

    @pl.when(shared)
    def _():
        for j in range(micro):
            which = order_ref[0, j]
            s0 = start_ref[0, which]
            spans[j, 0] = jnp.full(spans.shape[2:], s0, jnp.int32)
            spans[j, 1] = jnp.full(spans.shape[2:], s0 + len_ref[0, which], jnp.int32)

            @pl.when(sec == 0)
            def _():
                xin[j] = x_ref[which]

    for j in range(micro):
        @pl.when(sec == relays[j])
        def _():
            xout[j] = x_ref[order_ref[0, j]]

    @pl.when(jnp.logical_not(shared))
    def _():
        own.start()

    o_copy.start()

    pl.semaphore_wait(barrier, len(near) + line)

    def span_of(c):
        return pl.ds(c * width, width)

    def hop(j, c):
        return pltpu.make_async_remote_copy(
            src_ref=xout.at[j, :, span_of(c)], dst_ref=xin.at[j, :, span_of(c)],
            send_sem=hop_send.at[j, c], recv_sem=hop_recv.at[j, c],
            device_id=(above, me), device_id_type=MESH,
        )

    row_id = lax.broadcasted_iota(jnp.int32, (seq, seq), 0)
    col_id = lax.broadcasted_iota(jnp.int32, (seq, seq), 1)

    def mask(s0, s1):
        return (col_id <= row_id) | (
            (row_id >= s0) & (row_id < s1) & (col_id >= s0) & (col_id < s1)
        )

    def remote(source, dest, sent, got, other, level=None):
        return pltpu.make_async_remote_copy(
            src_ref=source, dst_ref=dest, send_sem=sent, recv_sem=got,
            device_id=(sec if level is None else level, other), device_id_type=MESH,
        )

    def hand_on(s, j, c):
        return remote(
            xout.at[j, :, span_of(c)], relay.at[s, j, :, span_of(c)],
            pass_send.at[s, j, c], pass_recv.at[s, j, c], mates[s],
        )

    def fall(s, j, c):
        return remote(
            relay.at[s, j, :, span_of(c)], xmate.at[s, j, :, span_of(c)],
            fall_send.at[s, j, c], x_recv.at[s, j, c], me, 0,
        )

    pieces = [(c, s) for c in range(chunks) for s in range(2)]

    def lift(j):
        @pl.when(sec == relays[j])
        def _():
            for c, s in pieces:
                hand_on(s, j, c).start()

    def drop(j):
        @pl.when(sec == relays[j])
        def _():
            for c, s in pieces:
                hand_on(s, j, c).wait_recv()
                fall(s, j, c).start()
            for c, s in pieces:
                hand_on(s, j, c).wait_send()

    low = [j for j in range(micro) if relays[j] < SHARED_SECTIONS]
    high = [j for j in range(micro) if relays[j] >= SHARED_SECTIONS]

    def out(j, g):
        first, size = runs(EXITS)[g]
        here = (j, slice(None), pl.ds(first * width, size * width))
        return pltpu.make_async_copy(xout.at[here], out_ref.at[here], out_sem.at[j, g])

    def leave(j, between=None):
        for g, (first, size) in enumerate(runs(EXITS)):
            if between is not None and 2 * first == chunks:
                between()
            span = slice(first * width, (first + size) * width)
            grown = jnp.dot(att[j], obuf[:, span], preferred_element_type=jnp.float32)
            fresh = (xin[j, :, span].astype(jnp.float32) + grown).astype(jnp.bfloat16)
            xout[j, :, span] = fresh
            out_ref[j, :, span] = fresh

            @pl.when(sec < sections - 1)
            def _():
                for c in range(first, first + size):
                    hop(j, c).start()

    def head(q, k, v, allowed):
        scores = lax.dot_general(
            q, k, (((1,), (1,)), ((), ())), preferred_element_type=jnp.float32
        )
        lifted = jnp.where(allowed, jnp.exp2(scores), 0.0)
        mixed = jnp.dot(
            lifted.astype(jnp.bfloat16), v.astype(jnp.bfloat16),
            preferred_element_type=jnp.float32,
        )
        return (mixed * (1.0 / jnp.sum(lifted, axis=-1, keepdims=True))).astype(jnp.bfloat16)

    def lifted_norm(p, scale, gain):
        mean = jnp.mean(p * p, axis=-1, keepdims=True) * scale * scale
        return (p * (lax.rsqrt(mean + EPS) * scale) * gain).astype(jnp.bfloat16)

    @pl.when(shared)
    def _():
        def swap(s, p):
            where = cols_of(flip(units[s]), p)
            return remote(
                w_ref.at[:, where], wbuf.at[own_rows, where],
                swap_send.at[s, p], swap_recv.at[s, p], mates[s],
            )

        def circle(s, k, b, p):
            where = cols_of(units[s], p)
            rows = block(seat(s, 1 - k, b == 1))
            source = w_ref.at[:, where] if k == 1 and b == 0 else wbuf.at[rows, where]
            return remote(
                source, wbuf.at[rows, where],
                loop_send.at[s, k - 1, b, p], loop_recv.at[s, k - 1, b, p], seat(s, 1, False),
            )

        def owner_of(s, i):
            return mates[s] if i == 0 else seat(s, -((i + 1) // 2), i % 2 == 0)

        def hand(s, i, p):
            here = wbuf.at[block(owner_of(s, i)), cols_of(units[s], p)]
            return remote(here, here, core_send.at[s, i, p], core_recv.at[s, i, p], partner)

        def mine(s, p):
            where = cols_of(units[s], p)
            return remote(
                w_ref.at[:, where], wbuf.at[own_rows, where],
                mine_send.at[s, p], mine_recv.at[s, p], partner,
            )

        def share(s, j, c):
            return remote(
                xin.at[j, :, span_of(c)], xmate.at[s, j, :, span_of(c)],
                x_send.at[s, j, c], x_recv.at[s, j, c], mates[s],
            )

        lot = quarter // RETURNS

        def give(s, j, n):
            return remote(
                ret.at[s, j, :, pl.ds(n * lot, lot)],
                att.at[j, :, aligned(units[s] * quarter + n * lot, lot)],
                give_send.at[s, j, n], give_recv.at[s, j, n], mates[s],
            )

        def tell(s):
            return remote(spans, mate_spans.at[s], span_send.at[s], span_recv.at[s], mates[s])

        both = [(p, s) for p in range(PARTS) for s in range(2)]
        waves = 2 * length - 1

        for s in range(2):
            tell(s).start()

        def climb(s):
            return remote(
                w_ref.at[:, cols_of(units[s], CARRIED)], wup.at[s],
                up_send.at[s], up_recv.at[s], me, CARRIER,
            )

        def cross(s):
            return remote(
                wup.at[s], wover.at[s], over_send.at[s], over_recv.at[s], seat(s, 1, False)
            )

        def sink(s):
            rows = block(seat(s, -1, False))
            return remote(
                wover.at[s], wbuf.at[rows, cols_of(units[s], CARRIED)],
                down_send.at[s], loop_recv.at[s, 0, 0, CARRIED], me, 0,
            )

        @pl.when(sec == 0)
        def _():
            for s in range(2):
                climb(s).start()

        for p, s in both[:4]:
            swap(s, p).start()
        for p, s in both:
            mine(s, p).start()

        @pl.when(sec == CARRIER)
        def _():
            for s in range(2):
                climb(s).wait_recv()
                cross(s).start()

        for j in low:
            lift(j)
        for p, s in both[4:]:
            swap(s, p).start()
        for p, s in both:
            if p == CARRIED:
                @pl.when(sec > 0)
                def _():
                    circle(s, 1, 0, p).start()
            else:
                circle(s, 1, 0, p).start()

        def fold(x):
            out = x[:, :128]
            for i in range(1, x.shape[1] // 128):
                out = out + x[:, i * 128 : (i + 1) * 128]
            return out

        def project(j, s, start, size, parts, fresh):
            here = aligned(start, size)
            gain = gain_ref[:, here]
            ours = xin[j, :, here].astype(jnp.float32)
            theirs = xmate[s, j, :, here].astype(jnp.float32)
            left = jnp.concatenate(
                [(ours * gain).astype(jnp.bfloat16), (theirs * gain).astype(jnp.bfloat16)], axis=0
            )
            for p in parts:
                cols = cols_of(units[s], p)
                part = jnp.dot(left, wbuf[here, cols], preferred_element_type=jnp.float32)
                if fresh:
                    acc[:, cols] = part
                else:
                    acc[:, cols] += part
            if 0 in parts:
                squares = [(1 + s, theirs)] + ([(0, ours)] if s == 0 else [])
                for k, x in squares:
                    if fresh:
                        ssq[k] = fold(x * x)
                    else:
                        ssq[k] += fold(x * x)

        chip_rows = 2 * shard

        def arrive(i, p):
            for s in range(2):
                if i == 0:
                    swap(s, p).wait_recv()
                    circle(s, 1, 1, p).start()
                else:
                    k, b = (i + 1) // 2, (i + 1) % 2
                    circle(s, k, b, p).wait_recv()
                    if k < length - 1:
                        circle(s, k + 1, b, p).start()
                hand(s, i, p).start()

        def finish(i, p):
            for s in range(2):
                hand(s, i, p).wait_recv()

            @pl.when(sec == 0)
            def _():
                for s in range(2):
                    start = lax.div(owner_of(s, i), 2) * chip_rows
                    project(0, s, start, chip_rows, (p,), False)

        for p in range(PARTS - 1):
            arrive(0, p)

        @pl.when(sec == CARRIER)
        def _():
            for s in range(2):
                cross(s).wait_recv()
                sink(s).start()

        for j in low:
            drop(j)
        arrive(0, PARTS - 1)
        for p, s in both:
            stay(s, p).wait()
            mine(s, p).wait_recv()

        @pl.when(sec == 0)
        def _():
            for c in range(chunks):
                for s in range(2):
                    share(s, 0, c).wait_recv()
            for s in range(2):
                project(0, s, chip * chip_rows, chip_rows, range(PARTS), True)

        for p in range(PARTS):
            finish(0, p)
        for i in range(1, waves):
            for p in range(PARTS):
                arrive(i, p)
                if p > 0:
                    finish(i, p - 1)
            finish(i, PARTS - 1)

        for s in range(2):
            tell(s).wait_recv()
        o_copy.wait()

        def ready(turn, region, unit, scale, heads):
            rows = slice(region * seq, (region + 1) * seq)
            for part, gains in ((0, qg_ref), (1, kg_ref)):
                factor = HEAD_DIM ** (-0.5) * LOG2_E if part == 0 else 1.0
                for i in heads:
                    start = unit * quarter + i * HEAD_DIM
                    p = acc[rows, aligned(part * model + start, HEAD_DIM)]
                    spot = (turn * 2 + part) * quarter + i * HEAD_DIM
                    qkv[:, spot : spot + HEAD_DIM] = lifted_norm(
                        p, scale, gains[:, aligned(start, HEAD_DIM)] * factor
                    )

        def attend(turn, region, unit, scale, allowed, heads, ref, base):
            ready(turn, region, unit, scale, heads)
            rows = slice(region * seq, (region + 1) * seq)
            for i in heads:
                spot = turn * 2 * quarter + i * HEAD_DIM
                v = acc[rows, aligned(2 * model + unit * quarter + i * HEAD_DIM, HEAD_DIM)] * scale
                ref[:, aligned(base + i * HEAD_DIM, HEAD_DIM)] = head(
                    qkv[:, spot : spot + HEAD_DIM],
                    qkv[:, spot + quarter : spot + quarter + HEAD_DIM], v, allowed,
                )

        def pass_on(j, c):
            hop(j, c).wait_recv()
            for s in range(2):
                share(s, j, c).start()

        @pl.loop(0, micro)
        def _(j):
            def ahead_of(n):
                for where, counts in ((sec == 1, EARLY[0]), (sec > 1, EARLY[1])):
                    if counts[n] > 0:
                        @pl.when(where & (j < micro - 1))
                        def _():
                            for c in range(sum(counts[:n]), sum(counts[: n + 1])):
                                pass_on(j + 1, c)

            @pl.when((sec > 0) | (j > 0))
            def _():
                def finish(first, size):
                    for c in range(first, first + size):
                        for s in range(2):
                            share(s, j, c).wait_recv()
                    for s in range(2):
                        project(j, s, first * width, size * width, range(PARTS), first == 0)

                for c in range(chunks + LAG):
                    if c < chunks:
                        late = ((sec == 1) & (c >= sum(EARLY[0]))) | ((sec > 1) & (c >= sum(EARLY[1])))

                        @pl.when((sec > 0) & ((j == 0) | late))
                        def _():
                            pass_on(j, c)

                    if c == chunks + LAG - 1:
                        ahead_of(0)
                    for first, size in runs(GROUPS):
                        if first + size == c - LAG + 1:
                            finish(first, size)

            def scale_of(k):
                square = jnp.sum(ssq[k], axis=-1, keepdims=True)
                return lax.rsqrt(square * (1.0 / model) + EPS)

            scales = [scale_of(1 + s) for s in range(2)]
            open_to = [
                mask(mate_spans[s, j, 0, 0:1, :], mate_spans[s, j, 1, 0:1, :]) for s in range(2)
            ]
            for n in range(RETURNS):
                heads = range(n * few // RETURNS, (n + 1) * few // RETURNS)
                for s in range(2):
                    attend(s, 1, units[s], scales[s], open_to[s], heads, ret.at[s, j], 0)
                for s in range(2):
                    give(s, j, n).start()

            ahead_of(1)
            which = order_ref[0, j]
            s0 = start_ref[0, which]
            allowed = mask(s0, s0 + len_ref[0, which])
            scale = scale_of(0)
            for s in range(2):
                attend(2 + s, 0, units[s], scale, allowed, range(few), att.at[j], units[s] * quarter)
            ahead_of(2)
            for n in range(RETURNS):
                for s in range(2):
                    give(s, j, n).wait_recv()
            ahead_of(3)
            leave(j, lambda: ahead_of(4))

        for s in range(2):
            tell(s).wait_send()
            for p in range(PARTS):
                swap(s, p).wait_send()
                mine(s, p).wait_send()
                for i in range(waves):
                    hand(s, i, p).wait_send()
                for k in range(1, length):
                    for b in range(2):
                        if (k, b, p) != (1, 0, CARRIED):
                            circle(s, k, b, p).wait_send()
            for j in range(micro):
                for n in range(RETURNS):
                    give(s, j, n).wait_send()

        @pl.when(sec > 0)
        def _():
            for s in range(2):
                circle(s, 1, 0, CARRIED).wait_send()
                for j in range(micro):
                    for c in range(chunks):
                        share(s, j, c).wait_send()

        @pl.when(sec == 0)
        def _():
            for s in range(2):
                climb(s).wait_send()

        @pl.when(sec == CARRIER)
        def _():
            for s in range(2):
                cross(s).wait_send()
                sink(s).wait_send()

    @pl.when(jnp.logical_not(shared))
    def _():
        def rows(owner, way, sub):
            return pl.ds(pl.multiple_of(owner * shard + (way * SUBS + sub) * piece, piece), piece)

        def ring_copy(way, sub, step):
            owner = at(-step if way == 0 else step)
            where = rows(owner, way, sub)
            if step == 0:
                source = w_ref.at[pl.ds((way * SUBS + sub) * piece, piece)]
            else:
                source = wbuf.at[where]
            return pltpu.make_async_remote_copy(
                src_ref=source, dst_ref=wbuf.at[where],
                send_sem=ring_send.at[way, sub, step], recv_sem=ring_recv.at[way, sub, step],
                device_id=(sec, ahead if way == 0 else behind), device_id_type=MESH,
            )

        def pair_copy(way, sub, step):
            owner = at(-step if way == 0 else step)
            where = rows(owner, way, sub)
            return pltpu.make_async_remote_copy(
                src_ref=wbuf.at[where], dst_ref=wbuf.at[where],
                send_sem=pair_send.at[way, sub, step - 1], recv_sem=pair_recv.at[way, sub, step - 1],
                device_id=(sec, partner), device_id_type=MESH,
            )

        for j in high:
            lift(j)
        ring = {}
        pair = {}
        for sub in range(SUBS):
            for way in range(2):
                ring[way, sub, 0] = ring_copy(way, sub, 0)
                ring[way, sub, 0].start()
        first = pltpu.make_async_remote_copy(
            src_ref=w_ref, dst_ref=wbuf.at[own_rows], send_sem=first_send, recv_sem=first_recv,
            device_id=(sec, partner), device_id_type=MESH,
        )
        first.start()
        for j in high:
            drop(j)
        own.wait()
        first.wait_recv()
        for step in range(1, chips):
            for sub in range(SUBS):
                for way in range(2):
                    ring[way, sub, step - 1].wait_recv()
                    if step < chips - 1:
                        ring[way, sub, step] = ring_copy(way, sub, step)
                        ring[way, sub, step].start()
                    pair[way, sub, step] = pair_copy(way, sub, step)
                    pair[way, sub, step].start()
            for way in range(2):
                for sub in range(SUBS):
                    pair[way, sub, step].wait_recv()
        o_copy.wait()
        first.wait_send()
        for step in range(1, chips):
            for sub in range(SUBS):
                for way in range(2):
                    pair[way, sub, step].wait_send()
                    ring[way, sub, step - 1].wait_send()

        @pl.loop(0, micro)
        def _(j):
            which = order_ref[0, j]
            s0 = start_ref[0, which]
            s1 = s0 + len_ref[0, which]
            here_rows = slice(0, seq)
            square = jnp.zeros((seq, 1), jnp.float32)
            for first, size in runs(GROUPS):
                span = slice(first * width, (first + size) * width)
                for c in range(first, first + size):
                    hop(j, c).wait_recv()
                wide = xin[j, :, span].astype(jnp.float32)
                square = square + jnp.sum(wide * wide, axis=-1, keepdims=True)
                scaled = (wide * gain_ref[:, span]).astype(jnp.bfloat16)
                part = jnp.dot(scaled, wbuf[span, :], preferred_element_type=jnp.float32)
                if first == 0:
                    acc[here_rows, :] = part
                else:
                    acc[here_rows, :] += part

            scale = lax.rsqrt(square * (1.0 / model) + EPS)

            for part, gains in ((0, qg_ref), (1, kg_ref)):
                factor = HEAD_DIM ** (-0.5) * LOG2_E if part == 0 else 1.0

                @pl.loop(0, model // (NORMS_AT_ONCE * HEAD_DIM))
                def _(n):
                    for i in range(NORMS_AT_ONCE):
                        base = (n * NORMS_AT_ONCE + i) * HEAD_DIM
                        here = pl.ds(pl.multiple_of(base, HEAD_DIM), HEAD_DIM)
                        cols = pl.ds(pl.multiple_of(part * model + base, HEAD_DIM), HEAD_DIM)
                        qkv[:, cols] = lifted_norm(acc[here_rows, cols], scale, gains[:, here] * factor)

            allowed = mask(s0, s1)

            @pl.loop(0, model // (HEADS_AT_ONCE * HEAD_DIM))
            def _(n):
                for i in range(HEADS_AT_ONCE):
                    base = (n * HEADS_AT_ONCE + i) * HEAD_DIM
                    here = pl.ds(pl.multiple_of(base, HEAD_DIM), HEAD_DIM)
                    q = qkv[:, here]
                    k = qkv[:, pl.ds(pl.multiple_of(model + base, HEAD_DIM), HEAD_DIM)]
                    v = acc[here_rows, pl.ds(pl.multiple_of(2 * model + base, HEAD_DIM), HEAD_DIM)] * scale
                    att[j, :, here] = head(q, k, v, allowed)

            leave(j)

    for j in range(micro):
        @pl.when(sec == relays[j])
        def _():
            for c, s in pieces:
                fall(s, j, c).wait_send()

    @pl.when(sec < sections - 1)
    def _():
        for j in range(micro):
            for c in range(chunks):
                hop(j, c).wait_send()


def solution(mesh):
    sections, devices = mesh.shape["section"], mesh.shape["dp"]

    def body(inputs, order, image_start, image_len, norm_gain, qkv_weight, q_gain, k_gain, o_weight):
        micro = order.shape[1]
        count, model = inputs.shape
        seq = count // micro
        total = qkv_weight.shape[2]
        shard = qkv_weight.shape[1]
        chunks = CHUNKS
        chips = devices // 2
        length = chips // 2
        smem = pl.BlockSpec(memory_space=pltpu.SMEM)
        vmem = pl.BlockSpec(memory_space=pltpu.VMEM)
        hbm = pl.BlockSpec(memory_space=pltpu.HBM)
        dma = pltpu.SemaphoreType.DMA
        out = pl.pallas_call(
            functools.partial(kernel, sections, devices),
            out_shape=pltpu.VMEM((micro, seq, model), jnp.bfloat16),
            in_specs=[smem, smem, smem, hbm, vmem, hbm, vmem, vmem, hbm],
            out_specs=vmem,
            scratch_shapes=[
                pltpu.VMEM((model, total), jnp.bfloat16),
                pltpu.VMEM((model, model), jnp.bfloat16),
                pltpu.VMEM((micro, seq, model), jnp.bfloat16),
                pltpu.VMEM((micro, seq, model), jnp.bfloat16),
                pltpu.VMEM((2 * seq, total), jnp.float32),
                pltpu.VMEM((seq, 2 * model), jnp.bfloat16),
                pltpu.VMEM((micro, seq, model), jnp.bfloat16),
                pltpu.VMEM((2, micro, seq, model), jnp.bfloat16),
                pltpu.VMEM((2, micro, seq, model), jnp.bfloat16),
                pltpu.VMEM((2, micro, seq, model // 4), jnp.bfloat16),
                pltpu.VMEM((3, seq, 128), jnp.float32),
                pltpu.VMEM((micro, 2, 8, 128), jnp.int32),
                pltpu.VMEM((2, micro, 2, 8, 128), jnp.int32),
                pltpu.VMEM((2, shard, model // 4), jnp.bfloat16),
                pltpu.VMEM((2, shard, model // 4), jnp.bfloat16),
                dma, dma, dma, dma,
                dma((2, SUBS, chips - 1)),
                dma((2, SUBS, chips - 1)),
                dma((2, SUBS, chips - 1)),
                dma((2, SUBS, chips - 1)),
                dma((micro, chunks)),
                dma((micro, chunks)),
                dma((2, PARTS)),
                dma((2, PARTS)),
                dma((2, PARTS)),
                dma((2, length - 1, 2, PARTS)),
                dma((2, length - 1, 2, PARTS)),
                dma((2, 2 * length - 1, PARTS)),
                dma((2, 2 * length - 1, PARTS)),
                dma((2, PARTS)),
                dma((2, PARTS)),
                dma((2, micro, chunks)),
                dma((2, micro, chunks)),
                dma((2, micro, RETURNS)),
                dma((2, micro, RETURNS)),
                dma((2,)),
                dma((2,)),
                dma((2, micro, CHUNKS)),
                dma((2, micro, CHUNKS)),
                dma((2, micro, CHUNKS)),
                dma((micro, len(EXITS))),
                dma((2,)),
                dma((2,)),
                dma((2,)),
                dma((2,)),
                dma((2,)),
                pltpu.VMEM((micro, seq, model), jnp.bfloat16),
                dma,
            ],
            compiler_params=pltpu.CompilerParams(
                collective_id=0, has_side_effects=True, vmem_limit_bytes=60 * 1024 * 1024
            ),
        )(
            order, image_start, image_len, inputs.reshape(micro, seq, model), norm_gain,
            qkv_weight.reshape(shard, total), q_gain, k_gain, o_weight.reshape(model, model),
        )
        return out.reshape(1, count, model)

    in_specs = (
        P("dp", None),
        P("dp", None),
        P("dp", None),
        P("dp", None),
        P("section", None),
        P("section", "dp", None),
        P("section", None),
        P("section", None),
        P("section", None, None),
    )
    out_specs = P("section", "dp", None)
    return jax.shard_map(body, mesh=mesh, in_specs=in_specs, out_specs=out_specs, check_vma=False)
```
